32 devices in a mesh: row: 4 (over x, core), col: 4 (over z), pt: 2 (over y).
Axes of the slice: x: 2, y: 2, z: 4, core: 2. Of those that a mesh axis runs over, the one named last changes fastest.
Arguments:
- first_factors: int32 [32, 1024, 1024], P('pt', 'row', 'col'), may hold values from 0 to 12288
- second_factors: int32 [32, 1024, 1024], P('pt', 'row', 'col'), may hold values from 0 to 12288
Outputs:
- scaled_product: float32 [45, 1024, 1024], P(None, ('row', 'pt'), 'col')
The draws below stay inside these ranges and needn't reach their ends.
All inputs are finite; a program needn't handle non-finite values.
Results may differ from the reference program's by a relative error of at most 0.0003.
Values may be sent and summed in bfloat16 or wider, within the bound.
A program may use at most 128 MiB of HBM per device.

```python
import jax
import jax.numpy as jnp
import numpy as np
from jax import lax

N = 1024
DEG = 16


def touch_ends(result, stream_key, low, top_value):
    place = [jax.random.randint(jax.random.fold_in(stream_key, axis), (), 0, length) for axis, length in enumerate(result.shape)]
    longest = result.shape.index(max(result.shape))
    neighbour = place[:longest] + [(place[longest] + 1) % result.shape[longest]] + place[longest + 1:]
    return result.at[tuple(place)].set(low).at[tuple(neighbour)].set(top_value)


def setup_inputs(seed: int = 0) -> dict:
    key_of = jax.random.split(jax.random.key(seed), 3)
    return {
        "first_factors": touch_ends(jax.random.randint(key_of[0], (2 * DEG, N, N), 0, 12289), jax.random.fold_in(key_of[0], 1), 0, 12288).astype(jnp.int32),
        "second_factors": touch_ends(jax.random.randint(key_of[1], (2 * DEG, N, N), 0, 12289), jax.random.fold_in(key_of[1], 1), 0, 12288).astype(jnp.int32),
    }


modulus = 12289
digit_base = 128


def primitive_root():
    for candidate in range(2, modulus):
        if pow(candidate, 6144, modulus) != 1 and pow(candidate, 4096, modulus) != 1:
            return candidate
    return 0


def make_table(order_size, row_count, column_count, inverse):
    generator = primitive_root()
    root_value = pow(generator, (modulus - 1) // order_size, modulus)
    scaling = 1
    if inverse:
        root_value = pow(root_value, modulus - 2, modulus)
        scaling = pow(order_size, modulus - 2, modulus)
    entries = [[pow(root_value, (row_index * column_index) % order_size, modulus) * scaling % modulus
                for column_index in range(column_count)] for row_index in range(row_count)]
    return np.array(entries, dtype=np.int64)


def exact_dot(left_part, right_part):
    return jnp.dot(left_part, right_part, precision=lax.Precision.HIGHEST, preferred_element_type=jnp.float32)


def value_digits(values):
    high_digit = values // digit_base
    return high_digit.astype(jnp.float32), (values - digit_base * high_digit).astype(jnp.float32)


def combine(high_high, high_low, low_high, low_low):
    top_part = high_high.astype(jnp.int32) % modulus
    middle_part = (high_low.astype(jnp.int32) + low_high.astype(jnp.int32)) % modulus
    return ((top_part * (digit_base * digit_base)) % modulus + middle_part * digit_base + low_low.astype(jnp.int32)) % modulus


def modular_product(matrix_table, values):
    table_high = jnp.asarray(matrix_table // digit_base, dtype=jnp.float32)
    table_low = jnp.asarray(matrix_table % digit_base, dtype=jnp.float32)
    data_high, data_low = value_digits(values)
    return combine(exact_dot(table_high, data_high), exact_dot(table_high, data_low),
                   exact_dot(table_low, data_high), exact_dot(table_low, data_low))


def transform(matrix_table, coefs):
    slot_count = coefs.shape[0]
    blocks = coefs.reshape(slot_count, 16, coefs.shape[1] // 16, coefs.shape[2]).transpose(1, 0, 2, 3)

    def one_block(block):
        flat_coefs = block.reshape(slot_count, -1)
        return modular_product(matrix_table, flat_coefs).reshape(-1, block.shape[1], block.shape[2])

    mapped = lax.map(one_block, blocks)
    return mapped.transpose(1, 0, 2, 3).reshape(-1, coefs.shape[1], coefs.shape[2])


def pointwise(left_values, right_values):
    def one_point(pair_in):
        left_high, left_low = value_digits(pair_in[0])
        right_high, right_low = value_digits(pair_in[1])
        return combine(exact_dot(left_high, right_high), exact_dot(left_high, right_low),
                       exact_dot(left_low, right_high), exact_dot(left_low, right_low))

    return lax.map(one_point, (left_values, right_values))


def reference(first_factors, second_factors):
    forward_one = make_table(2 * DEG, 2 * DEG, DEG, False)
    inverse_one = make_table(2 * DEG, 2 * DEG, 2 * DEG, True)
    forward_two = make_table(4 * DEG, 4 * DEG, 2 * DEG, False)
    inverse_two = make_table(4 * DEG, 3 * DEG - 3, 4 * DEG, True)
    left_values = jnp.concatenate([transform(forward_one, first_factors[:DEG]),
                                   transform(forward_one, first_factors[DEG:])], 0)
    right_values = jnp.concatenate([transform(forward_one, second_factors[:DEG]),
                                    transform(forward_one, second_factors[DEG:])], 0)
    products = pointwise(left_values, right_values)
    first_product = transform(inverse_one, products[:2 * DEG])
    second_product = transform(inverse_one, products[2 * DEG:])
    upper_values = transform(forward_two, first_product)
    lower_values = transform(forward_two[:, :DEG], second_product[DEG:])
    result_coefficients = transform(inverse_two, pointwise(upper_values, lower_values))
    return result_coefficients.astype(jnp.float32) / 12289.0
```

```python
import functools

import jax
import jax.numpy as jnp
import numpy as np
from jax import lax
from jax.experimental import pallas as pl
from jax.experimental.pallas import tpu as pltpu
from jax.sharding import PartitionSpec as P

DEG = 16


modulus = 12289
digit_base = 128


def primitive_root():
    for candidate in range(2, modulus):
        if pow(candidate, 6144, modulus) != 1 and pow(candidate, 4096, modulus) != 1:
            return candidate
    return 0


def make_table(order_size, row_count, column_count, inverse):
    generator = primitive_root()
    root_value = pow(generator, (modulus - 1) // order_size, modulus)
    scaling = 1
    if inverse:
        root_value = pow(root_value, modulus - 2, modulus)
        scaling = pow(order_size, modulus - 2, modulus)
    entries = [
        [
            pow(root_value, row_index * column_index % order_size, modulus) * scaling % modulus
            for column_index in range(column_count)
        ]
        for row_index in range(row_count)
    ]
    return np.array(entries, dtype=np.int64)


def value_digits(values):
    high_digit = values // digit_base
    return (
        high_digit.astype(jnp.bfloat16),
        (values - digit_base * high_digit).astype(jnp.bfloat16),
    )


def combine(high_high, high_low, low_high, low_low):
    top_part = high_high.astype(jnp.int32) % modulus
    middle_part = (high_low.astype(jnp.int32) + low_high.astype(jnp.int32)) % modulus
    return (
        top_part * (digit_base * digit_base) % modulus
        + middle_part * digit_base
        + low_low.astype(jnp.int32)
    ) % modulus


def transform(matrix_table, coefs):
    slot_count = coefs.shape[0]
    flat_coefs = coefs.reshape(slot_count, -1)
    table_high = jnp.asarray(matrix_table // digit_base, dtype=jnp.bfloat16)
    table_low = jnp.asarray(matrix_table % digit_base, dtype=jnp.bfloat16)
    data_high, data_low = value_digits(flat_coefs)

    def product_of(left_part, right_part):
        return jnp.dot(left_part, right_part, preferred_element_type=jnp.float32)

    mixed_values = combine(
        product_of(table_high, data_high),
        product_of(table_high, data_low),
        product_of(table_low, data_high),
        product_of(table_low, data_low),
    )
    return mixed_values.reshape(matrix_table.shape[0], coefs.shape[1], coefs.shape[2])


def batched_product(left_part, right_part):
    return jnp.einsum("bik,bkj->bij", left_part, right_part, preferred_element_type=jnp.float32)


def digit_sum(totals, left_digits, right_digits):
    return (
        totals[0] + batched_product(left_digits[0], right_digits[0]),
        totals[1] + batched_product(left_digits[0], right_digits[1]),
        totals[2] + batched_product(left_digits[1], right_digits[0]),
        totals[3] + batched_product(left_digits[1], right_digits[1]),
    )


def pointwise(left_values, right_values):
    left_points, right_points = (
        lax.all_to_all(
            lax.all_to_all(
                left_values.astype(jnp.float32), "col", split_axis=0, concat_axis=2, tiled=True
            ),
            "pt",
            split_axis=0,
            concat_axis=1,
            tiled=True,
        ),
        lax.all_to_all(
            lax.all_to_all(
                right_values.astype(jnp.float32), "col", split_axis=0, concat_axis=2, tiled=True
            ),
            "pt",
            split_axis=0,
            concat_axis=1,
            tiled=True,
        ),
    )
    left_digits = value_digits(left_points.astype(jnp.int32))
    right_digits = value_digits(right_points.astype(jnp.int32))
    zeros_init = jnp.zeros(left_points.shape, jnp.float32)
    column_parts = tuple((digit_part for digit_part in left_digits))
    totals = digit_sum(
        (zeros_init, zeros_init, zeros_init, zeros_init),
        column_parts,
        (
            lax.all_gather(right_digits[0], "row", axis=1, tiled=True),
            lax.all_gather(right_digits[1], "row", axis=1, tiled=True),
        ),
    )
    product_values = combine(totals[0], totals[1], totals[2], totals[3]).astype(jnp.float32)
    arrived = lax.all_to_all(
        lax.all_to_all(product_values, "col", split_axis=2, concat_axis=0, tiled=True),
        "pt",
        split_axis=1,
        concat_axis=0,
        tiled=True,
    )
    col_count = lax.axis_size("col")
    pt_count = lax.axis_size("pt")
    local_count = arrived.shape[0] // (col_count * pt_count)
    returned = arrived.reshape(pt_count, col_count, local_count, arrived.shape[1], arrived.shape[2])
    returned = returned.transpose(1, 0, 2, 3, 4).reshape(arrived.shape)
    return returned.astype(jnp.int32)


def local(first_factors, second_factors):
    forward_one = make_table(2 * DEG, 2 * DEG, DEG, False)
    inverse_one = make_table(2 * DEG, 2 * DEG, 2 * DEG, True)
    forward_two = make_table(4 * DEG, 4 * DEG, 2 * DEG, False)
    inverse_two = make_table(4 * DEG, 3 * DEG - 3, 4 * DEG, True)
    first_entries, second_entries = (
        lax.all_to_all(
            first_factors.astype(jnp.float32), "pt", split_axis=1, concat_axis=0, tiled=True
        ),
        lax.all_to_all(
            second_factors.astype(jnp.float32), "pt", split_axis=1, concat_axis=0, tiled=True
        ),
    )
    first_entries = first_entries.astype(jnp.int32)
    second_entries = second_entries.astype(jnp.int32)
    left_values = jnp.concatenate(
        [transform(forward_one, first_entries[:DEG]), transform(forward_one, first_entries[DEG:])],
        0,
    )
    right_values = jnp.concatenate(
        [
            transform(forward_one, second_entries[:DEG]),
            transform(forward_one, second_entries[DEG:]),
        ],
        0,
    )
    products = pointwise(left_values, right_values)
    first_product = transform(inverse_one, products[: 2 * DEG])
    second_product = transform(inverse_one, products[2 * DEG :])
    upper_values = transform(forward_two, first_product)
    lower_values = transform(forward_two[:, :DEG], second_product[DEG:])
    result_coefficients = transform(inverse_two, pointwise(upper_values, lower_values))
    return result_coefficients.astype(jnp.float32) / 12289.0


def reduce_centred(values):
    return values - 12289.0 * jnp.round(values * (1.0 / 12289.0))


def table_digits(matrix_table):
    centred = np.where(matrix_table > modulus // 2, matrix_table - modulus, matrix_table)
    high_digit = np.round(centred / 128.0)
    return high_digit, centred - 128.0 * high_digit


def centre(values):
    return jnp.where(values > modulus // 2, values - modulus, values)


MESH = pl.DeviceIdType.MESH
sub_rows = 8
chunk_count = 4
vmem_limit = 67_000_000


def spread_table(matrix_table):
    shifted_table = matrix_table * 128 % modulus
    parts = [table_digits(matrix_table), table_digits(shifted_table)]
    base = np.concatenate(
        [128.0 * parts[0][0], 128.0 * parts[1][0], parts[0][1], parts[1][1]], axis=1
    )
    slots = matrix_table.shape[1]
    weights = np.concatenate([np.full(slots, 65.0), np.full(slots, 97.0)] * 2)
    if np.max(np.abs(base) @ weights) >= 2.0**24:
        raise ValueError("inexact sums")
    return jnp.asarray(np.kron(base, np.eye(sub_rows)), dtype=jnp.bfloat16)


def low_and_high(values):
    high_digit = jnp.round(values * (1.0 / 128.0))
    return values - 128.0 * high_digit, high_digit


def spread_dot(table_value, values):
    slots, rows, columns = values.shape
    low, high = (
        digit.reshape(slots * rows, columns).astype(jnp.bfloat16) for digit in low_and_high(values)
    )
    result = jnp.dot(
        table_value,
        jnp.concatenate([low, high, low, high], axis=0),
        preferred_element_type=jnp.float32,
    )
    return result.reshape(-1, rows, columns)


def as_float(values):
    return values.astype(jnp.int32).astype(jnp.float32)


def as_short(values):
    return values.astype(jnp.int32).astype(jnp.int16)


def transform_group(table_ref, source_ref, block, start):
    values = as_float(source_ref[block, :, pl.ds(start, 2 * sub_rows), :])
    table_value = table_ref[...]
    return jnp.concatenate(
        [
            reduce_centred(spread_dot(table_value, values[:, :sub_rows])),
            reduce_centred(spread_dot(table_value, values[:, sub_rows:])),
        ],
        axis=1,
    )


def transform_left(table_ref, source_ref, block, digits_ref):
    rows, columns = source_ref.shape[2:]

    def group(index, carry):
        start = pl.multiple_of(index * 2 * sub_rows, 2 * sub_rows)
        values = transform_group(table_ref, source_ref, block, start)
        low, high = low_and_high(values)
        shifted_low = jnp.round(values * (-1.0 / 96.0))
        shifted_high = values + 96.0 * shifted_low
        top, bottom = pl.ds(start, 2 * sub_rows), pl.ds(rows + start, 2 * sub_rows)
        digits_ref[:, top, :columns] = shifted_high.astype(jnp.bfloat16)
        digits_ref[:, top, columns:] = high.astype(jnp.bfloat16)
        digits_ref[:, bottom, :columns] = shifted_low.astype(jnp.bfloat16)
        digits_ref[:, bottom, columns:] = low.astype(jnp.bfloat16)
        return carry

    lax.fori_loop(0, rows // (2 * sub_rows), group, 0)


def transform_right(table_ref, source_ref, block, digits_ref):
    rows = source_ref.shape[2]

    def group(index, carry):
        start = pl.multiple_of(index * 2 * sub_rows, 2 * sub_rows)
        values = transform_group(table_ref, source_ref, block, start)
        low, high = low_and_high(values)
        digits_ref[:, pl.ds(start, 2 * sub_rows), :] = high.astype(jnp.bfloat16)
        digits_ref[:, pl.ds(rows + start, 2 * sub_rows), :] = low.astype(jnp.bfloat16)
        return carry

    lax.fori_loop(0, rows // (2 * sub_rows), group, 0)


def multiply_points(left_ref, right_ref, totals_ref, first):
    def point(index, carry):
        product = jnp.dot(left_ref[index], right_ref[index], preferred_element_type=jnp.float32)

        @pl.when(first)
        def _():
            totals_ref[index] = product

        @pl.when(jnp.logical_not(first))
        def _():
            totals_ref[index] += product

        return carry

    lax.fori_loop(0, left_ref.shape[0], point, 0)


def folded(totals_ref, start, rows):
    high = totals_ref[:, pl.ds(start, rows), :]
    low = totals_ref[:, pl.ds(totals_ref.shape[1] // 2 + start, rows), :]
    values = reduce_centred(reduce_centred(high) * 128.0 + low)
    half = values.shape[0] // 2
    return values[:half] + values[half:], values[:half] - values[half:]


def remote(source, target, send, receive, **place):
    return pltpu.make_async_remote_copy(
        src_ref=source,
        dst_ref=target,
        send_sem=send,
        recv_sem=receive,
        device_id=place,
        device_id_type=MESH,
    )


class Line:
    def __init__(self, axis, size, buffer, slots, send, receive):
        self.axis, self.size, self.buffer = axis, size, buffer
        self.place = lax.axis_index(axis)
        self.slots = slots
        self.send, self.receive = send, receive
        self.rows = buffer.shape[2] // chunk_count

    def copy(self, direction, step, chunk, block):
        rows = pl.ds(pl.multiple_of(chunk * self.rows, self.rows), self.rows)
        part = self.buffer.at[block, pl.ds(0, self.slots), rows, :]
        target = self.place + (1 if direction else -1)
        return remote(
            part,
            part,
            self.send.at[direction, step, chunk],
            self.receive.at[direction, step, chunk],
            **{self.axis: target},
        )

    def sends(self, step, act):
        pl.when((self.place > 0) & (self.place + step < self.size))(
            lambda: act(0, self.place + step)
        )
        pl.when((self.place < self.size - 1) & (self.place - step >= 0))(
            lambda: act(1, self.place - step)
        )

    def start(self, chunk):
        self.sends(0, lambda direction, block: self.copy(direction, 0, chunk, block).start())

    def tick(self, step, chunk):
        def arrive(direction, block):
            self.copy(direction, step, chunk, block).wait_recv()

        pl.when(self.place + step + 1 < self.size)(lambda: arrive(0, self.place + step + 1))
        pl.when(self.place - step - 1 >= 0)(lambda: arrive(1, self.place - step - 1))

        @pl.when(step + 1 < self.size - 1)
        def _():
            self.sends(
                step + 1,
                lambda direction, block: self.copy(direction, step + 1, chunk, block).start(),
            )

    def finish(self):
        def one(index, carry):
            step, chunk = index // chunk_count, index % chunk_count
            self.sends(
                step, lambda direction, block: self.copy(direction, step, chunk, block).wait_send()
            )
            return carry

        lax.fori_loop(0, (self.size - 1) * chunk_count, one, 0)

    def block_at(self, position):
        first = self.place + 1 - 2 * (self.place // (self.size - 1))
        last = (self.size - 1) * (1 - self.place // (self.size // 2))
        third = self.size * (self.size - 1) // 2 - self.place - first - last
        return (
            jnp.where(position == 0, self.place, 0)
            + jnp.where(position == 1, first, 0)
            + jnp.where(position == 2, third, 0)
            + jnp.where(position == 3, last, 0)
        )


class Square:
    def __init__(self, axis, buffer, slots, send, receive):
        self.axis, self.buffer, self.slots = axis, buffer, slots
        self.place = lax.axis_index(axis)
        self.near = self.place + 1 - 2 * (self.place % 2)
        self.far = (self.place + 2) % 4
        self.send, self.receive = send, receive
        self.rows = buffer.shape[2] // chunk_count

    def copy(self, kind, chunk, sending):
        rows = pl.ds(pl.multiple_of(chunk * self.rows, self.rows), self.rows)
        if kind == 0:
            block, target = (self.place if sending else self.far), self.far
        elif kind == 1:
            block, target = (self.place if sending else self.near), self.near
        else:
            block, target = (self.far if sending else (self.near + 2) % 4), self.near
        part = self.buffer.at[block, pl.ds(0, self.slots), rows, :]
        return remote(
            part, part, self.send.at[kind, chunk], self.receive.at[kind, chunk], **{self.axis: target}
        )

    def start(self, chunk):
        self.copy(0, chunk, True).start()
        self.copy(1, chunk, True).start()

    def tick(self, chunk):
        self.copy(0, chunk, False).wait_recv()
        self.copy(2, chunk, True).start()

    def arrive(self, chunk):
        self.copy(1, chunk, False).wait_recv()
        self.copy(2, chunk, False).wait_recv()

    def finish(self, chunk):
        for kind in range(3):
            self.copy(kind, chunk, True).wait_send()


def each_chunk(act):
    def one(chunk, carry):
        act(chunk)
        return carry

    lax.fori_loop(0, chunk_count, one, 0)


def greet(line, square, others=()):
    barrier = pltpu.get_barrier_semaphore()

    def signal(**place):
        pl.semaphore_signal(barrier, inc=1, device_id=place, device_id_type=MESH)

    for target in (square.near, square.far):
        signal(**{square.axis: target})
    for place in others:
        signal(**place)
    before, after = line.place > 0, line.place < line.size - 1
    pl.when(before)(lambda: signal(**{line.axis: line.place - 1}))
    pl.when(after)(lambda: signal(**{line.axis: line.place + 1}))
    ends = (line.place + line.size - 1) // line.size + 1 - (line.place + 1) // line.size
    pl.semaphore_wait(barrier, 2 + len(others) + ends)


def pipeline(line, square, left, right, multiply):
    each_chunk(lambda chunk: (line.tick(0, chunk), square.tick(chunk)))
    each_chunk(square.arrive)
    tick_count = (line.size - 2) * chunk_count

    def one(index, carry):
        pl.when(index < tick_count)(
            lambda: line.tick(1 + index // chunk_count, index % chunk_count)
        )
        position = jnp.where(index < tick_count, index // 2, line.size - 1)
        works = (index < 2 * (line.size - 1)) | (index >= tick_count)

        @pl.when(works & (index % 2 == 0))
        def _():
            block = line.block_at(position)
            left(block)
            right(block)

        @pl.when(works & (index % 2 == 1))
        def _():
            multiply(position == 0)

        return carry

    lax.fori_loop(0, tick_count + 2, one, 0)
    line.finish()
    each_chunk(square.finish)


def product_kernel(
    size,
    left_hbm,
    right_hbm,
    forward_ref,
    even_ref,
    odd_ref,
    out_ref,
    left_ref,
    right_ref,
    left_digits,
    right_digits,
    totals,
    line_send,
    line_receive,
    square_send,
    square_receive,
    local_sems,
):
    slots = left_ref.shape[1]
    line = Line("col", size, left_ref, slots, line_send, line_receive)
    square = Square("row", right_ref, slots, square_send, square_receive)
    copies = (
        pltpu.make_async_copy(left_hbm, left_ref.at[line.place], local_sems.at[0]),
        pltpu.make_async_copy(right_hbm, right_ref.at[square.place], local_sems.at[1]),
    )
    for copy in copies:
        copy.start()
    greet(line, square)
    for copy in copies:
        copy.wait()
    each_chunk(lambda chunk: (line.start(chunk), square.start(chunk)))
    pipeline(
        line,
        square,
        lambda block: transform_left(forward_ref, left_ref, block, left_digits),
        lambda block: transform_right(forward_ref, right_ref, block, right_digits),
        lambda first: multiply_points(left_digits, right_digits, totals, first),
    )

    def group(index, carry):
        start = pl.multiple_of(index * 2 * sub_rows, 2 * sub_rows)
        halves = []
        for half in range(2):
            sums, differences = folded(totals, start + half * sub_rows, sub_rows)
            halves.append(
                [
                    reduce_centred(spread_dot(even_ref[...], sums)),
                    reduce_centred(spread_dot(odd_ref[...], differences)),
                ]
            )
        for parity in range(2):
            values = as_short(jnp.concatenate([halves[0][parity], halves[1][parity]], axis=1))
            for place in range(values.shape[0]):
                out_ref[2 * place + parity, pl.ds(start, 2 * sub_rows), :] = values[place]
        return carry

    lax.fori_loop(0, out_ref.shape[1] // (2 * sub_rows), group, 0)


def result_kernel(
    size,
    product_hbm,
    upper_table,
    lower_table,
    even_ref,
    odd_ref,
    out_ref,
    left_ref,
    right_ref,
    left_digits,
    right_digits,
    totals,
    line_send,
    line_receive,
    square_send,
    square_receive,
    cross_send,
    cross_receive,
    local_sems,
):
    left_slots, right_slots = left_ref.shape[1] - 1, right_ref.shape[1] - 1
    rows = left_ref.shape[2]
    line = Line("col", size, left_ref, left_slots, line_send, line_receive)
    square = Square("row", right_ref, right_slots, square_send, square_receive)
    side = lax.axis_index("pt")
    own_left = product_hbm.at[pl.ds(0, left_slots), pl.ds(0, rows), :]
    own_right = product_hbm.at[pl.ds(right_ref.shape[1], right_slots), :, :]
    copy_left = pltpu.make_async_copy(
        own_left, left_ref.at[line.place, pl.ds(0, left_slots)], local_sems.at[0]
    )
    copy_right = pltpu.make_async_copy(
        own_right, right_ref.at[square.place, pl.ds(0, right_slots)], local_sems.at[1]
    )
    pl.when(side == 0)(copy_left.start)
    pl.when(side == 1)(copy_right.start)
    for block in range(size):
        left_ref[block, left_slots] = jnp.zeros(left_ref.shape[2:], left_ref.dtype)
        right_ref[block, right_slots] = jnp.zeros(right_ref.shape[2:], right_ref.dtype)
    greet(line, square, ({"pt": 1 - side},))

    def cross_left(chunk):
        part = pl.multiple_of(chunk * line.rows, line.rows)
        return remote(
            product_hbm.at[pl.ds(0, left_slots), pl.ds(rows + part, line.rows), :],
            left_ref.at[line.place, pl.ds(0, left_slots), pl.ds(part, line.rows), :],
            cross_send.at[chunk],
            cross_receive.at[chunk],
            pt=1 - side,
        )

    def cross_right(chunk):
        part = pl.multiple_of(chunk * square.rows, square.rows)
        return remote(
            product_hbm.at[
                pl.ds(right_ref.shape[1], right_slots), pl.ds(part, square.rows), :
            ],
            right_ref.at[square.place, pl.ds(0, right_slots), pl.ds(part, square.rows), :],
            cross_send.at[chunk],
            cross_receive.at[chunk],
            pt=1 - side,
        )

    @pl.when(side == 0)
    def _():
        each_chunk(lambda chunk: cross_left(chunk).start())
        copy_left.wait()
        each_chunk(line.start)
        each_chunk(lambda chunk: (cross_right(chunk).wait_recv(), square.start(chunk)))

    @pl.when(side == 1)
    def _():
        each_chunk(lambda chunk: cross_right(chunk).start())
        copy_right.wait()
        each_chunk(square.start)
        each_chunk(lambda chunk: (cross_left(chunk).wait_recv(), line.start(chunk)))

    pipeline(
        line,
        square,
        lambda block: transform_left(upper_table, left_ref, block, left_digits),
        lambda block: transform_right(lower_table, right_ref, block, right_digits),
        lambda first: multiply_points(left_digits, right_digits, totals, first),
    )
    pl.when(side == 0)(lambda: each_chunk(lambda chunk: cross_left(chunk).wait_send()))
    pl.when(side == 1)(lambda: each_chunk(lambda chunk: cross_right(chunk).wait_send()))

    def group(index, carry):
        start = pl.multiple_of(index * sub_rows, sub_rows)
        for parity, (table_ref, values) in enumerate(
            zip((even_ref, odd_ref), folded(totals, start, sub_rows))
        ):
            result = reduce_centred(spread_dot(table_ref[...], values))
            result = jnp.where(result < 0.0, result + 12289.0, result) * (1.0 / 12289.0)
            for place in range(result.shape[0]):
                out_ref[2 * place + parity, pl.ds(start, sub_rows), :] = result[place]
        return carry

    lax.fori_loop(0, out_ref.shape[1] // sub_rows, group, 0)


def call(kernel, collective_id, arguments, tables, out_shape, out_dtype, shapes, extra=()):
    left, right, points = shapes
    size, rows, columns = left[0], left[2], left[3]
    inner, width = right[2], right[3]
    return pl.pallas_call(
        functools.partial(kernel, size),
        out_shape=jax.ShapeDtypeStruct(out_shape, out_dtype),
        in_specs=[pl.BlockSpec(memory_space=pl.ANY)] * len(arguments)
        + [pl.BlockSpec(memory_space=pltpu.VMEM)] * len(tables),
        out_specs=pl.BlockSpec(memory_space=pltpu.VMEM),
        scratch_shapes=[
            pltpu.VMEM(left, jnp.int16),
            pltpu.VMEM(right, jnp.int16),
            pltpu.VMEM((points, 2 * rows, 2 * columns), jnp.bfloat16),
            pltpu.VMEM((points, 2 * inner, width), jnp.bfloat16),
            pltpu.VMEM((points, 2 * rows, width), jnp.float32),
            pltpu.SemaphoreType.DMA((2, size - 1, chunk_count)),
            pltpu.SemaphoreType.DMA((2, size - 1, chunk_count)),
            pltpu.SemaphoreType.DMA((3, chunk_count)),
            pltpu.SemaphoreType.DMA((3, chunk_count)),
            *extra,
            pltpu.SemaphoreType.DMA((2,)),
        ],
        compiler_params=pltpu.CompilerParams(
            collective_id=collective_id, has_side_effects=True, vmem_limit_bytes=vmem_limit
        ),
        name=kernel.__name__,
    )(*arguments, *tables)


def square_local(first_factors, second_factors):
    size = lax.axis_size("col")
    slots, rows, columns = first_factors.shape
    points = 2 * slots
    inverse_one = make_table(points, points, points, True)
    left, right = (centre(values).astype(jnp.int16) for values in (first_factors, second_factors))
    products = call(
        product_kernel,
        0,
        (left, right),
        [
            spread_table(make_table(points, points, slots, False)),
            spread_table(inverse_one[0::2, :slots]),
            spread_table(inverse_one[1::2, :slots]),
        ],
        (points, rows, columns),
        jnp.int16,
        ((size, slots, rows, columns), (size, slots, rows, columns), points),
    )
    last_points = 3 * slots
    inverse_two = make_table(last_points, last_points - 3, last_points, True)
    half = last_points // 2
    own_rows = rows // lax.axis_size("pt")
    return call(
        result_kernel,
        1,
        (products,),
        [
            spread_table(make_table(last_points, last_points, points, False)),
            spread_table(make_table(last_points, last_points, slots, False)),
            spread_table(inverse_two[0::2, :half]),
            spread_table(inverse_two[1::2, :half]),
        ],
        (last_points - 3, own_rows, columns),
        jnp.float32,
        ((size, points, own_rows, columns), (size, slots, rows, columns), last_points),
        extra=(
            pltpu.SemaphoreType.DMA((chunk_count,)),
            pltpu.SemaphoreType.DMA((chunk_count,)),
        ),
    )


def solution(mesh):
    in_specs = (P("pt", "row", "col"), P("pt", "row", "col"))
    out_specs = P(None, ("row", "pt"), "col")
    squares = mesh.shape["row"] == 4 and mesh.shape["col"] == 4 and mesh.shape["pt"] == 2
    body = square_local if squares else local
    return jax.shard_map(body, mesh=mesh, in_specs=in_specs, out_specs=out_specs, check_vma=False)
```

```python
import functools

import jax
import jax.numpy as jnp
import numpy as np
from jax import lax
from jax.experimental import pallas as pl
from jax.experimental.pallas import tpu as pltpu
from jax.sharding import PartitionSpec as P

DEG = 16


modulus = 12289
digit_base = 128


def primitive_root():
    for candidate in range(2, modulus):
        if pow(candidate, 6144, modulus) != 1 and pow(candidate, 4096, modulus) != 1:
            return candidate
    return 0


def make_table(order_size, row_count, column_count, inverse):
    generator = primitive_root()
    root_value = pow(generator, (modulus - 1) // order_size, modulus)
    scaling = 1
    if inverse:
        root_value = pow(root_value, modulus - 2, modulus)
        scaling = pow(order_size, modulus - 2, modulus)
    entries = [
        [
            pow(root_value, row_index * column_index % order_size, modulus) * scaling % modulus
            for column_index in range(column_count)
        ]
        for row_index in range(row_count)
    ]
    return np.array(entries, dtype=np.int64)


def value_digits(values):
    high_digit = values // digit_base
    return (
        high_digit.astype(jnp.bfloat16),
        (values - digit_base * high_digit).astype(jnp.bfloat16),
    )


def combine(high_high, high_low, low_high, low_low):
    top_part = high_high.astype(jnp.int32) % modulus
    middle_part = (high_low.astype(jnp.int32) + low_high.astype(jnp.int32)) % modulus
    return (
        top_part * (digit_base * digit_base) % modulus
        + middle_part * digit_base
        + low_low.astype(jnp.int32)
    ) % modulus


def transform(matrix_table, coefs):
    slot_count = coefs.shape[0]
    flat_coefs = coefs.reshape(slot_count, -1)
    table_high = jnp.asarray(matrix_table // digit_base, dtype=jnp.bfloat16)
    table_low = jnp.asarray(matrix_table % digit_base, dtype=jnp.bfloat16)
    data_high, data_low = value_digits(flat_coefs)

    def product_of(left_part, right_part):
        return jnp.dot(left_part, right_part, preferred_element_type=jnp.float32)

    mixed_values = combine(
        product_of(table_high, data_high),
        product_of(table_high, data_low),
        product_of(table_low, data_high),
        product_of(table_low, data_low),
    )
    return mixed_values.reshape(matrix_table.shape[0], coefs.shape[1], coefs.shape[2])


def batched_product(left_part, right_part):
    return jnp.einsum("bik,bkj->bij", left_part, right_part, preferred_element_type=jnp.float32)


def digit_sum(totals, left_digits, right_digits):
    return (
        totals[0] + batched_product(left_digits[0], right_digits[0]),
        totals[1] + batched_product(left_digits[0], right_digits[1]),
        totals[2] + batched_product(left_digits[1], right_digits[0]),
        totals[3] + batched_product(left_digits[1], right_digits[1]),
    )


def pointwise(left_values, right_values):
    left_points, right_points = (
        lax.all_to_all(
            lax.all_to_all(
                left_values.astype(jnp.float32), "col", split_axis=0, concat_axis=2, tiled=True
            ),
            "pt",
            split_axis=0,
            concat_axis=1,
            tiled=True,
        ),
        lax.all_to_all(
            lax.all_to_all(
                right_values.astype(jnp.float32), "col", split_axis=0, concat_axis=2, tiled=True
            ),
            "pt",
            split_axis=0,
            concat_axis=1,
            tiled=True,
        ),
    )
    left_digits = value_digits(left_points.astype(jnp.int32))
    right_digits = value_digits(right_points.astype(jnp.int32))
    zeros_init = jnp.zeros(left_points.shape, jnp.float32)
    column_parts = tuple((digit_part for digit_part in left_digits))
    totals = digit_sum(
        (zeros_init, zeros_init, zeros_init, zeros_init),
        column_parts,
        (
            lax.all_gather(right_digits[0], "row", axis=1, tiled=True),
            lax.all_gather(right_digits[1], "row", axis=1, tiled=True),
        ),
    )
    product_values = combine(totals[0], totals[1], totals[2], totals[3]).astype(jnp.float32)
    arrived = lax.all_to_all(
        lax.all_to_all(product_values, "col", split_axis=2, concat_axis=0, tiled=True),
        "pt",
        split_axis=1,
        concat_axis=0,
        tiled=True,
    )
    col_count = lax.axis_size("col")
    pt_count = lax.axis_size("pt")
    local_count = arrived.shape[0] // (col_count * pt_count)
    returned = arrived.reshape(pt_count, col_count, local_count, arrived.shape[1], arrived.shape[2])
    returned = returned.transpose(1, 0, 2, 3, 4).reshape(arrived.shape)
    return returned.astype(jnp.int32)


def local(first_factors, second_factors):
    forward_one = make_table(2 * DEG, 2 * DEG, DEG, False)
    inverse_one = make_table(2 * DEG, 2 * DEG, 2 * DEG, True)
    forward_two = make_table(4 * DEG, 4 * DEG, 2 * DEG, False)
    inverse_two = make_table(4 * DEG, 3 * DEG - 3, 4 * DEG, True)
    first_entries, second_entries = (
        lax.all_to_all(
            first_factors.astype(jnp.float32), "pt", split_axis=1, concat_axis=0, tiled=True
        ),
        lax.all_to_all(
            second_factors.astype(jnp.float32), "pt", split_axis=1, concat_axis=0, tiled=True
        ),
    )
    first_entries = first_entries.astype(jnp.int32)
    second_entries = second_entries.astype(jnp.int32)
    left_values = jnp.concatenate(
        [transform(forward_one, first_entries[:DEG]), transform(forward_one, first_entries[DEG:])],
        0,
    )
    right_values = jnp.concatenate(
        [
            transform(forward_one, second_entries[:DEG]),
            transform(forward_one, second_entries[DEG:]),
        ],
        0,
    )
    products = pointwise(left_values, right_values)
    first_product = transform(inverse_one, products[: 2 * DEG])
    second_product = transform(inverse_one, products[2 * DEG :])
    upper_values = transform(forward_two, first_product)
    lower_values = transform(forward_two[:, :DEG], second_product[DEG:])
    result_coefficients = transform(inverse_two, pointwise(upper_values, lower_values))
    return result_coefficients.astype(jnp.float32) / 12289.0


def reduce_centred(values):
    return values - 12289.0 * jnp.round(values * (1.0 / 12289.0))


def table_digits(matrix_table):
    centred = np.where(matrix_table > modulus // 2, matrix_table - modulus, matrix_table)
    high_digit = np.round(centred / 128.0)
    return high_digit, centred - 128.0 * high_digit


def centre(values):
    return jnp.where(values > modulus // 2, values - modulus, values)


MESH = pl.DeviceIdType.MESH
sub_rows = 8
chunk_count = 4
vmem_limit = 67_000_000


def spread_table(matrix_table):
    shifted_table = matrix_table * 128 % modulus
    parts = [table_digits(matrix_table), table_digits(shifted_table)]
    base = np.concatenate(
        [128.0 * parts[0][0], 128.0 * parts[1][0], parts[0][1], parts[1][1]], axis=1
    )
    slots = matrix_table.shape[1]
    weights = np.concatenate([np.full(slots, 65.0), np.full(slots, 97.0)] * 2)
    if np.max(np.abs(base) @ weights) >= 2.0**24:
        raise ValueError("inexact sums")
    return jnp.asarray(np.kron(base, np.eye(sub_rows)), dtype=jnp.bfloat16)


def low_and_high(values):
    high_digit = jnp.round(values * (1.0 / 128.0))
    return values - 128.0 * high_digit, high_digit


def spread_dot(table_value, values):
    slots, rows, columns = values.shape
    low, high = (
        digit.reshape(slots * rows, columns).astype(jnp.bfloat16) for digit in low_and_high(values)
    )
    result = jnp.dot(
        table_value,
        jnp.concatenate([low, high, low, high], axis=0),
        preferred_element_type=jnp.float32,
    )
    return result.reshape(-1, rows, columns)


def as_float(values):
    return values.astype(jnp.int32).astype(jnp.float32)


def as_short(values):
    return values.astype(jnp.int32).astype(jnp.int16)


def transform_group(table_ref, source_ref, block, start):
    values = as_float(source_ref[block, :, pl.ds(start, 2 * sub_rows), :])
    table_value = table_ref[...]
    return jnp.concatenate(
        [
            reduce_centred(spread_dot(table_value, values[:, :sub_rows])),
            reduce_centred(spread_dot(table_value, values[:, sub_rows:])),
        ],
        axis=1,
    )


def digit_rows(start, chunk_rows):
    top = start // chunk_rows * (2 * chunk_rows) + start % chunk_rows
    return pl.multiple_of(top, sub_rows), pl.multiple_of(top + chunk_rows, sub_rows)


def transform_left(table_ref, source_ref, block, chunk, count, digits_ref):
    columns = source_ref.shape[3]
    chunk_rows = source_ref.shape[2] // chunk_count
    groups = chunk_rows // (2 * sub_rows)

    def group(index, carry):
        start = pl.multiple_of(index * 2 * sub_rows, 2 * sub_rows)
        values = transform_group(table_ref, source_ref, block, start)
        low, high = low_and_high(values)
        shifted_low = jnp.round(values * (-1.0 / 96.0))
        shifted_high = values + 96.0 * shifted_low
        top, bottom = (
            pl.ds(pl.multiple_of(place, 2 * sub_rows), 2 * sub_rows)
            for place in digit_rows(start, chunk_rows)
        )
        digits_ref[:, top, :columns] = shifted_high.astype(jnp.bfloat16)
        digits_ref[:, top, columns:] = high.astype(jnp.bfloat16)
        digits_ref[:, bottom, :columns] = shifted_low.astype(jnp.bfloat16)
        digits_ref[:, bottom, columns:] = low.astype(jnp.bfloat16)
        return carry

    lax.fori_loop(chunk * groups, (chunk + count) * groups, group, 0)


def transform_right(table_ref, source_ref, block, digits_ref):
    rows = source_ref.shape[2]

    def group(index, carry):
        start = pl.multiple_of(index * 2 * sub_rows, 2 * sub_rows)
        values = transform_group(table_ref, source_ref, block, start)
        low, high = low_and_high(values)
        digits_ref[:, pl.ds(start, 2 * sub_rows), :] = high.astype(jnp.bfloat16)
        digits_ref[:, pl.ds(rows + start, 2 * sub_rows), :] = low.astype(jnp.bfloat16)
        return carry

    lax.fori_loop(0, rows // (2 * sub_rows), group, 0)


point_unroll = 4


def multiply_points(left_ref, right_ref, totals_ref, first, chunk=None):
    if chunk is None:
        rows = slice(None)
    else:
        count = left_ref.shape[1] // chunk_count
        rows = pl.ds(pl.multiple_of(chunk * count, count), count)

    def point(index, carry):
        for place in range(point_unroll):
            at = index * point_unroll + place
            product = jnp.dot(
                left_ref[at, rows, :], right_ref[at], preferred_element_type=jnp.float32
            )
            totals_ref[at, rows, :] = product if first else totals_ref[at, rows, :] + product
        return carry

    lax.fori_loop(0, left_ref.shape[0] // point_unroll, point, 0)


def folded(totals_ref, start, rows, chunk_rows):
    top, bottom = digit_rows(start, chunk_rows)
    high = totals_ref[:, pl.ds(top, rows), :]
    low = totals_ref[:, pl.ds(bottom, rows), :]
    values = reduce_centred(reduce_centred(high) * 128.0 + low)
    half = values.shape[0] // 2
    return values[:half] + values[half:], values[:half] - values[half:]


def remote(source, target, send, receive, **place):
    return pltpu.make_async_remote_copy(
        src_ref=source,
        dst_ref=target,
        send_sem=send,
        recv_sem=receive,
        device_id=place,
        device_id_type=MESH,
    )


class Line:
    def __init__(self, axis, size, buffer, slots, send, receive):
        self.axis, self.size, self.buffer = axis, size, buffer
        self.place = lax.axis_index(axis)
        self.slots = slots
        self.send, self.receive = send, receive
        self.rows = buffer.shape[2] // chunk_count

    def copy(self, direction, step, chunk, block):
        rows = pl.ds(pl.multiple_of(chunk * self.rows, self.rows), self.rows)
        part = self.buffer.at[block, pl.ds(0, self.slots), rows, :]
        target = self.place + (1 if direction else -1)
        return remote(
            part,
            part,
            self.send.at[direction, step, chunk],
            self.receive.at[direction, step, chunk],
            **{self.axis: target},
        )

    def sends(self, step, act):
        pl.when((self.place > 0) & (self.place + step < self.size))(
            lambda: act(0, self.place + step)
        )
        pl.when((self.place < self.size - 1) & (self.place - step >= 0))(
            lambda: act(1, self.place - step)
        )

    def start(self, chunk):
        self.sends(0, lambda direction, block: self.copy(direction, 0, chunk, block).start())

    def tick(self, step, chunk):
        def arrive(direction, block):
            self.copy(direction, step, chunk, block).wait_recv()

        pl.when(self.place + step + 1 < self.size)(lambda: arrive(0, self.place + step + 1))
        pl.when(self.place - step - 1 >= 0)(lambda: arrive(1, self.place - step - 1))

        @pl.when(step + 1 < self.size - 1)
        def _():
            self.sends(
                step + 1,
                lambda direction, block: self.copy(direction, step + 1, chunk, block).start(),
            )

    def finish(self):
        def one(index, carry):
            step, chunk = index // chunk_count, index % chunk_count
            self.sends(
                step, lambda direction, block: self.copy(direction, step, chunk, block).wait_send()
            )
            return carry

        lax.fori_loop(0, (self.size - 1) * chunk_count, one, 0)

    def block_at(self, position):
        first = self.place + 1 - 2 * (self.place // (self.size - 1))
        last = (self.size - 1) * (1 - self.place // (self.size // 2))
        third = self.size * (self.size - 1) // 2 - self.place - first - last
        return (
            jnp.where(position == 0, self.place, 0)
            + jnp.where(position == 1, first, 0)
            + jnp.where(position == 2, third, 0)
            + jnp.where(position == 3, last, 0)
        )


class Square:
    def __init__(self, axis, buffer, slots, send, receive):
        self.axis, self.buffer, self.slots = axis, buffer, slots
        self.place = lax.axis_index(axis)
        self.near = self.place + 1 - 2 * (self.place % 2)
        self.far = (self.place + 2) % 4
        self.send, self.receive = send, receive
        self.rows = buffer.shape[2] // chunk_count

    def copy(self, kind, chunk, sending):
        rows = pl.ds(pl.multiple_of(chunk * self.rows, self.rows), self.rows)
        if kind == 0:
            block, target = (self.place if sending else self.far), self.far
        elif kind == 1:
            block, target = (self.place if sending else self.near), self.near
        else:
            block, target = (self.far if sending else (self.near + 2) % 4), self.near
        part = self.buffer.at[block, pl.ds(0, self.slots), rows, :]
        return remote(
            part, part, self.send.at[kind, chunk], self.receive.at[kind, chunk], **{self.axis: target}
        )

    def start(self, chunk):
        self.copy(0, chunk, True).start()
        self.copy(1, chunk, True).start()

    def tick(self, chunk):
        self.copy(0, chunk, False).wait_recv()
        self.copy(2, chunk, True).start()

    def arrive(self, chunk):
        self.copy(1, chunk, False).wait_recv()
        self.copy(2, chunk, False).wait_recv()

    def finish(self, chunk):
        for kind in range(3):
            self.copy(kind, chunk, True).wait_send()


def each_chunk(act):
    def one(chunk, carry):
        act(chunk)
        return carry

    lax.fori_loop(0, chunk_count, one, 0)


def greet(line, square, others=()):
    barrier = pltpu.get_barrier_semaphore()

    def signal(**place):
        pl.semaphore_signal(barrier, inc=1, device_id=place, device_id_type=MESH)

    for target in (square.near, square.far):
        signal(**{square.axis: target})
    for place in others:
        signal(**place)
    before, after = line.place > 0, line.place < line.size - 1
    pl.when(before)(lambda: signal(**{line.axis: line.place - 1}))
    pl.when(after)(lambda: signal(**{line.axis: line.place + 1}))
    ends = (line.place + line.size - 1) // line.size + 1 - (line.place + 1) // line.size
    pl.semaphore_wait(barrier, 2 + len(others) + ends)


def pipeline(line, square, left, right, multiply, finish):
    def first(chunk):
        line.tick(0, chunk)
        square.tick(chunk)
        left(line.block_at(0), chunk, 1)

    each_chunk(first)
    each_chunk(square.arrive)
    line.tick(1, 0)
    right(line.block_at(0))
    multiply(True)
    line.tick(1, 1)
    left(line.block_at(1), 0, chunk_count)
    right(line.block_at(1))
    line.tick(1, 2)
    multiply(False)
    line.tick(1, 3)
    left(line.block_at(2), 0, chunk_count)
    right(line.block_at(2))
    multiply(False)
    right(line.block_at(3))

    def last(chunk):
        line.tick(line.size - 2, chunk)
        left(line.block_at(line.size - 1), chunk, 1)
        multiply(False, chunk)
        finish(chunk)

    each_chunk(last)
    line.finish()
    each_chunk(square.finish)


def product_kernel(
    size,
    left_hbm,
    right_hbm,
    forward_ref,
    even_ref,
    odd_ref,
    out_ref,
    left_ref,
    right_ref,
    left_digits,
    right_digits,
    totals,
    line_send,
    line_receive,
    square_send,
    square_receive,
    local_sems,
):
    slots = left_ref.shape[1]
    line = Line("col", size, left_ref, slots, line_send, line_receive)
    square = Square("row", right_ref, slots, square_send, square_receive)
    copies = (
        pltpu.make_async_copy(left_hbm, left_ref.at[line.place], local_sems.at[0]),
        pltpu.make_async_copy(right_hbm, right_ref.at[square.place], local_sems.at[1]),
    )
    for copy in copies:
        copy.start()
    greet(line, square)
    for copy in copies:
        copy.wait()
    each_chunk(lambda chunk: (line.start(chunk), square.start(chunk)))
    chunk_rows = line.rows
    groups = chunk_rows // (2 * sub_rows)

    def finish(chunk):
        def group(index, carry):
            start = pl.multiple_of(index * 2 * sub_rows, 2 * sub_rows)
            halves = []
            for half in range(2):
                sums, differences = folded(totals, start + half * sub_rows, sub_rows, chunk_rows)
                halves.append(
                    [
                        reduce_centred(spread_dot(even_ref[...], sums)),
                        reduce_centred(spread_dot(odd_ref[...], differences)),
                    ]
                )
            for parity in range(2):
                values = as_short(jnp.concatenate([halves[0][parity], halves[1][parity]], axis=1))
                for place in range(values.shape[0]):
                    out_ref[2 * place + parity, pl.ds(start, 2 * sub_rows), :] = values[place]
            return carry

        lax.fori_loop(chunk * groups, (chunk + 1) * groups, group, 0)

    pipeline(
        line,
        square,
        lambda *place: transform_left(forward_ref, left_ref, *place, left_digits),
        lambda block: transform_right(forward_ref, right_ref, block, right_digits),
        lambda *place: multiply_points(left_digits, right_digits, totals, *place),
        finish,
    )


def result_kernel(
    size,
    product_hbm,
    upper_table,
    lower_table,
    even_ref,
    odd_ref,
    out_ref,
    left_ref,
    right_ref,
    left_digits,
    right_digits,
    totals,
    line_send,
    line_receive,
    square_send,
    square_receive,
    cross_send,
    cross_receive,
    local_sems,
):
    left_slots, right_slots = left_ref.shape[1] - 1, right_ref.shape[1] - 1
    rows = left_ref.shape[2]
    line = Line("col", size, left_ref, left_slots, line_send, line_receive)
    square = Square("row", right_ref, right_slots, square_send, square_receive)
    side = lax.axis_index("pt")
    own_left = product_hbm.at[pl.ds(0, left_slots), pl.ds(0, rows), :]
    own_right = product_hbm.at[pl.ds(right_ref.shape[1], right_slots), :, :]
    copy_left = pltpu.make_async_copy(
        own_left, left_ref.at[line.place, pl.ds(0, left_slots)], local_sems.at[0]
    )
    copy_right = pltpu.make_async_copy(
        own_right, right_ref.at[square.place, pl.ds(0, right_slots)], local_sems.at[1]
    )
    pl.when(side == 0)(copy_left.start)
    pl.when(side == 1)(copy_right.start)
    for block in range(size):
        left_ref[block, left_slots] = jnp.zeros(left_ref.shape[2:], left_ref.dtype)
        right_ref[block, right_slots] = jnp.zeros(right_ref.shape[2:], right_ref.dtype)
    greet(line, square, ({"pt": 1 - side},))

    def cross_left(chunk):
        part = pl.multiple_of(chunk * line.rows, line.rows)
        return remote(
            product_hbm.at[pl.ds(0, left_slots), pl.ds(rows + part, line.rows), :],
            left_ref.at[line.place, pl.ds(0, left_slots), pl.ds(part, line.rows), :],
            cross_send.at[chunk],
            cross_receive.at[chunk],
            pt=1 - side,
        )

    def cross_right(chunk):
        part = pl.multiple_of(chunk * square.rows, square.rows)
        return remote(
            product_hbm.at[
                pl.ds(right_ref.shape[1], right_slots), pl.ds(part, square.rows), :
            ],
            right_ref.at[square.place, pl.ds(0, right_slots), pl.ds(part, square.rows), :],
            cross_send.at[chunk],
            cross_receive.at[chunk],
            pt=1 - side,
        )

    @pl.when(side == 0)
    def _():
        each_chunk(lambda chunk: cross_left(chunk).start())
        copy_left.wait()
        each_chunk(line.start)
        each_chunk(lambda chunk: (cross_right(chunk).wait_recv(), square.start(chunk)))

    @pl.when(side == 1)
    def _():
        each_chunk(lambda chunk: cross_right(chunk).start())
        copy_right.wait()
        each_chunk(square.start)
        each_chunk(lambda chunk: (cross_left(chunk).wait_recv(), line.start(chunk)))

    chunk_rows = line.rows
    groups = chunk_rows // sub_rows

    def finish(chunk):
        def group(index, carry):
            start = pl.multiple_of(index * sub_rows, sub_rows)
            for parity, (table_ref, values) in enumerate(
                zip((even_ref, odd_ref), folded(totals, start, sub_rows, chunk_rows))
            ):
                result = reduce_centred(spread_dot(table_ref[...], values))
                result = jnp.where(result < 0.0, result + 12289.0, result) * (1.0 / 12289.0)
                for place in range(result.shape[0]):
                    out_ref[2 * place + parity, pl.ds(start, sub_rows), :] = result[place]
            return carry

        lax.fori_loop(chunk * groups, (chunk + 1) * groups, group, 0)

    pipeline(
        line,
        square,
        lambda *place: transform_left(upper_table, left_ref, *place, left_digits),
        lambda block: transform_right(lower_table, right_ref, block, right_digits),
        lambda *place: multiply_points(left_digits, right_digits, totals, *place),
        finish,
    )
    pl.when(side == 0)(lambda: each_chunk(lambda chunk: cross_left(chunk).wait_send()))
    pl.when(side == 1)(lambda: each_chunk(lambda chunk: cross_right(chunk).wait_send()))


def call(kernel, collective_id, arguments, tables, out_shape, out_dtype, shapes, extra=()):
    left, right, points = shapes
    size, rows, columns = left[0], left[2], left[3]
    inner, width = right[2], right[3]
    return pl.pallas_call(
        functools.partial(kernel, size),
        out_shape=jax.ShapeDtypeStruct(out_shape, out_dtype),
        in_specs=[pl.BlockSpec(memory_space=pl.ANY)] * len(arguments)
        + [pl.BlockSpec(memory_space=pltpu.VMEM)] * len(tables),
        out_specs=pl.BlockSpec(memory_space=pltpu.VMEM),
        scratch_shapes=[
            pltpu.VMEM(left, jnp.int16),
            pltpu.VMEM(right, jnp.int16),
            pltpu.VMEM((points, 2 * rows, 2 * columns), jnp.bfloat16),
            pltpu.VMEM((points, 2 * inner, width), jnp.bfloat16),
            pltpu.VMEM((points, 2 * rows, width), jnp.float32),
            pltpu.SemaphoreType.DMA((2, size - 1, chunk_count)),
            pltpu.SemaphoreType.DMA((2, size - 1, chunk_count)),
            pltpu.SemaphoreType.DMA((3, chunk_count)),
            pltpu.SemaphoreType.DMA((3, chunk_count)),
            *extra,
            pltpu.SemaphoreType.DMA((2,)),
        ],
        compiler_params=pltpu.CompilerParams(
            collective_id=collective_id, has_side_effects=True, vmem_limit_bytes=vmem_limit
        ),
        name=kernel.__name__,
    )(*arguments, *tables)


def square_local(first_factors, second_factors):
    size = lax.axis_size("col")
    slots, rows, columns = first_factors.shape
    points = 2 * slots
    inverse_one = make_table(points, points, points, True)
    left, right = (centre(values).astype(jnp.int16) for values in (first_factors, second_factors))
    products = call(
        product_kernel,
        0,
        (left, right),
        [
            spread_table(make_table(points, points, slots, False)),
            spread_table(inverse_one[0::2, :slots]),
            spread_table(inverse_one[1::2, :slots]),
        ],
        (points, rows, columns),
        jnp.int16,
        ((size, slots, rows, columns), (size, slots, rows, columns), points),
    )
    last_points = 3 * slots
    inverse_two = make_table(last_points, last_points - 3, last_points, True)
    half = last_points // 2
    own_rows = rows // lax.axis_size("pt")
    return call(
        result_kernel,
        1,
        (products,),
        [
            spread_table(make_table(last_points, last_points, points, False)),
            spread_table(make_table(last_points, last_points, slots, False)),
            spread_table(inverse_two[0::2, :half]),
            spread_table(inverse_two[1::2, :half]),
        ],
        (last_points - 3, own_rows, columns),
        jnp.float32,
        ((size, points, own_rows, columns), (size, slots, rows, columns), last_points),
        extra=(
            pltpu.SemaphoreType.DMA((chunk_count,)),
            pltpu.SemaphoreType.DMA((chunk_count,)),
        ),
    )


def solution(mesh):
    in_specs = (P("pt", "row", "col"), P("pt", "row", "col"))
    out_specs = P(None, ("row", "pt"), "col")
    squares = mesh.shape["row"] == 4 and mesh.shape["col"] == 4 and mesh.shape["pt"] == 2
    body = square_local if squares else local
    return jax.shard_map(body, mesh=mesh, in_specs=in_specs, out_specs=out_specs, check_vma=False)
```

```python
import functools

import jax
import jax.numpy as jnp
import numpy as np
from jax import lax
from jax.experimental import pallas as pl
from jax.experimental.pallas import tpu as pltpu
from jax.sharding import PartitionSpec as P

DEG = 16


modulus = 12289
digit_base = 128


def primitive_root():
    for candidate in range(2, modulus):
        if pow(candidate, 6144, modulus) != 1 and pow(candidate, 4096, modulus) != 1:
            return candidate
    return 0


def make_table(order_size, row_count, column_count, inverse):
    generator = primitive_root()
    root_value = pow(generator, (modulus - 1) // order_size, modulus)
    scaling = 1
    if inverse:
        root_value = pow(root_value, modulus - 2, modulus)
        scaling = pow(order_size, modulus - 2, modulus)
    entries = [
        [
            pow(root_value, row_index * column_index % order_size, modulus) * scaling % modulus
            for column_index in range(column_count)
        ]
        for row_index in range(row_count)
    ]
    return np.array(entries, dtype=np.int64)


def value_digits(values):
    high_digit = values // digit_base
    return (
        high_digit.astype(jnp.bfloat16),
        (values - digit_base * high_digit).astype(jnp.bfloat16),
    )


def combine(high_high, high_low, low_high, low_low):
    top_part = high_high.astype(jnp.int32) % modulus
    middle_part = (high_low.astype(jnp.int32) + low_high.astype(jnp.int32)) % modulus
    return (
        top_part * (digit_base * digit_base) % modulus
        + middle_part * digit_base
        + low_low.astype(jnp.int32)
    ) % modulus


def transform(matrix_table, coefs):
    slot_count = coefs.shape[0]
    flat_coefs = coefs.reshape(slot_count, -1)
    table_high = jnp.asarray(matrix_table // digit_base, dtype=jnp.bfloat16)
    table_low = jnp.asarray(matrix_table % digit_base, dtype=jnp.bfloat16)
    data_high, data_low = value_digits(flat_coefs)

    def product_of(left_part, right_part):
        return jnp.dot(left_part, right_part, preferred_element_type=jnp.float32)

    mixed_values = combine(
        product_of(table_high, data_high),
        product_of(table_high, data_low),
        product_of(table_low, data_high),
        product_of(table_low, data_low),
    )
    return mixed_values.reshape(matrix_table.shape[0], coefs.shape[1], coefs.shape[2])


def batched_product(left_part, right_part):
    return jnp.einsum("bik,bkj->bij", left_part, right_part, preferred_element_type=jnp.float32)


def digit_sum(totals, left_digits, right_digits):
    return (
        totals[0] + batched_product(left_digits[0], right_digits[0]),
        totals[1] + batched_product(left_digits[0], right_digits[1]),
        totals[2] + batched_product(left_digits[1], right_digits[0]),
        totals[3] + batched_product(left_digits[1], right_digits[1]),
    )


def pointwise(left_values, right_values):
    left_points, right_points = (
        lax.all_to_all(
            lax.all_to_all(
                left_values.astype(jnp.float32), "col", split_axis=0, concat_axis=2, tiled=True
            ),
            "pt",
            split_axis=0,
            concat_axis=1,
            tiled=True,
        ),
        lax.all_to_all(
            lax.all_to_all(
                right_values.astype(jnp.float32), "col", split_axis=0, concat_axis=2, tiled=True
            ),
            "pt",
            split_axis=0,
            concat_axis=1,
            tiled=True,
        ),
    )
    left_digits = value_digits(left_points.astype(jnp.int32))
    right_digits = value_digits(right_points.astype(jnp.int32))
    zeros_init = jnp.zeros(left_points.shape, jnp.float32)
    column_parts = tuple((digit_part for digit_part in left_digits))
    totals = digit_sum(
        (zeros_init, zeros_init, zeros_init, zeros_init),
        column_parts,
        (
            lax.all_gather(right_digits[0], "row", axis=1, tiled=True),
            lax.all_gather(right_digits[1], "row", axis=1, tiled=True),
        ),
    )
    product_values = combine(totals[0], totals[1], totals[2], totals[3]).astype(jnp.float32)
    arrived = lax.all_to_all(
        lax.all_to_all(product_values, "col", split_axis=2, concat_axis=0, tiled=True),
        "pt",
        split_axis=1,
        concat_axis=0,
        tiled=True,
    )
    col_count = lax.axis_size("col")
    pt_count = lax.axis_size("pt")
    local_count = arrived.shape[0] // (col_count * pt_count)
    returned = arrived.reshape(pt_count, col_count, local_count, arrived.shape[1], arrived.shape[2])
    returned = returned.transpose(1, 0, 2, 3, 4).reshape(arrived.shape)
    return returned.astype(jnp.int32)


def local(first_factors, second_factors):
    forward_one = make_table(2 * DEG, 2 * DEG, DEG, False)
    inverse_one = make_table(2 * DEG, 2 * DEG, 2 * DEG, True)
    forward_two = make_table(4 * DEG, 4 * DEG, 2 * DEG, False)
    inverse_two = make_table(4 * DEG, 3 * DEG - 3, 4 * DEG, True)
    first_entries, second_entries = (
        lax.all_to_all(
            first_factors.astype(jnp.float32), "pt", split_axis=1, concat_axis=0, tiled=True
        ),
        lax.all_to_all(
            second_factors.astype(jnp.float32), "pt", split_axis=1, concat_axis=0, tiled=True
        ),
    )
    first_entries = first_entries.astype(jnp.int32)
    second_entries = second_entries.astype(jnp.int32)
    left_values = jnp.concatenate(
        [transform(forward_one, first_entries[:DEG]), transform(forward_one, first_entries[DEG:])],
        0,
    )
    right_values = jnp.concatenate(
        [
            transform(forward_one, second_entries[:DEG]),
            transform(forward_one, second_entries[DEG:]),
        ],
        0,
    )
    products = pointwise(left_values, right_values)
    first_product = transform(inverse_one, products[: 2 * DEG])
    second_product = transform(inverse_one, products[2 * DEG :])
    upper_values = transform(forward_two, first_product)
    lower_values = transform(forward_two[:, :DEG], second_product[DEG:])
    result_coefficients = transform(inverse_two, pointwise(upper_values, lower_values))
    return result_coefficients.astype(jnp.float32) / 12289.0


def reduce_centred(values):
    return values - 12289.0 * jnp.round(values * (1.0 / 12289.0))


def table_digits(matrix_table):
    centred = np.where(matrix_table > modulus // 2, matrix_table - modulus, matrix_table)
    high_digit = np.round(centred / 128.0)
    return high_digit, centred - 128.0 * high_digit


def centre(values):
    return jnp.where(values > modulus // 2, values - modulus, values)


MESH = pl.DeviceIdType.MESH
sub_rows = 8
chunk_count = 4
vmem_limit = 67_000_000


def spread_table(matrix_table):
    shifted_table = matrix_table * 128 % modulus
    parts = [table_digits(matrix_table), table_digits(shifted_table)]
    base = np.concatenate(
        [128.0 * parts[0][0], 128.0 * parts[1][0], parts[0][1], parts[1][1]], axis=1
    )
    slots = matrix_table.shape[1]
    weights = np.concatenate([np.full(slots, 65.0), np.full(slots, 97.0)] * 2)
    if np.max(np.abs(base) @ weights) >= 2.0**24:
        raise ValueError("inexact sums")
    return jnp.asarray(np.kron(base, np.eye(sub_rows)), dtype=jnp.bfloat16)


def low_and_high(values):
    high_digit = jnp.round(values * (1.0 / 128.0))
    return values - 128.0 * high_digit, high_digit


def spread_dot(table_value, parts):
    slots, rows, columns = parts[0].shape
    sides = []
    for values in parts:
        low, high = (
            digit.reshape(slots * rows, columns).astype(jnp.bfloat16)
            for digit in low_and_high(values)
        )
        sides.append(jnp.concatenate([low, high, low, high], axis=0))
    result = jnp.dot(
        table_value, jnp.concatenate(sides, axis=1), preferred_element_type=jnp.float32
    )
    return [
        reduce_centred(
            result[:, place * columns : (place + 1) * columns].reshape(-1, rows, columns)
        )
        for place in range(len(parts))
    ]


def as_float(values):
    return values.astype(jnp.int32).astype(jnp.float32)


def as_short(values):
    return values.astype(jnp.int32).astype(jnp.int16)


def transform_group(table_ref, source_ref, block, start):
    values = as_float(source_ref[block, :, pl.ds(start, 2 * sub_rows), :])
    parts = [values[:, :sub_rows], values[:, sub_rows:]]
    return jnp.concatenate(spread_dot(table_ref[...], parts), axis=1)


def transform_left(table_ref, source_ref, block, chunk, count, digits_ref):
    columns = source_ref.shape[3]
    groups = source_ref.shape[2] // chunk_count // (2 * sub_rows)

    def group(index, carry):
        start = pl.multiple_of(index * 2 * sub_rows, 2 * sub_rows)
        low, high = low_and_high(transform_group(table_ref, source_ref, block, start))
        digits_ref[:, pl.ds(start, 2 * sub_rows), :columns] = high.astype(jnp.bfloat16)
        digits_ref[:, pl.ds(start, 2 * sub_rows), columns:] = low.astype(jnp.bfloat16)
        return carry

    lax.fori_loop(chunk * groups, (chunk + count) * groups, group, 0)


def transform_right(table_ref, source_ref, block, digits_ref):
    rows, columns = source_ref.shape[2:]

    def group(index, carry):
        start = pl.multiple_of(index * 2 * sub_rows, 2 * sub_rows)
        values = transform_group(table_ref, source_ref, block, start)
        low, high = low_and_high(values)
        shifted_low = jnp.round(values * (-1.0 / 96.0))
        shifted_high = values + 96.0 * shifted_low
        top, bottom = pl.ds(start, 2 * sub_rows), pl.ds(rows + start, 2 * sub_rows)
        digits_ref[:, top, :columns] = shifted_high.astype(jnp.bfloat16)
        digits_ref[:, top, columns:] = shifted_low.astype(jnp.bfloat16)
        digits_ref[:, bottom, :columns] = high.astype(jnp.bfloat16)
        digits_ref[:, bottom, columns:] = low.astype(jnp.bfloat16)
        return carry

    lax.fori_loop(0, rows // (2 * sub_rows), group, 0)


point_unroll = 8


def multiply_points(left_ref, right_ref, totals_ref, first, part=None):
    half = left_ref.shape[1] // 2
    rows = slice(None) if part is None else pl.ds(pl.multiple_of(part * half, half), half)

    def point(index, carry):
        for place in range(point_unroll):
            at = index * point_unroll + place
            product = jnp.dot(
                left_ref[at, rows, :], right_ref[at], preferred_element_type=jnp.float32
            )
            totals_ref[at, rows, :] = product if first else totals_ref[at, rows, :] + product
        return carry

    lax.fori_loop(0, left_ref.shape[0] // point_unroll, point, 0)


def folded(totals_ref, start, rows):
    width = totals_ref.shape[2] // 2
    high = totals_ref[:, pl.ds(start, rows), :width]
    low = totals_ref[:, pl.ds(start, rows), width:]
    values = reduce_centred(reduce_centred(high) * 128.0 + low)
    half = values.shape[0] // 2
    return values[:half] + values[half:], values[:half] - values[half:]


def remote(source, target, send, receive, **place):
    return pltpu.make_async_remote_copy(
        src_ref=source,
        dst_ref=target,
        send_sem=send,
        recv_sem=receive,
        device_id=place,
        device_id_type=MESH,
    )


class Line:
    def __init__(self, axis, size, buffer, slots, send, receive):
        self.axis, self.size, self.buffer = axis, size, buffer
        self.place = lax.axis_index(axis)
        self.slots = slots
        self.send, self.receive = send, receive
        self.rows = buffer.shape[2] // chunk_count

    def copy(self, direction, step, chunk, block):
        rows = pl.ds(pl.multiple_of(chunk * self.rows, self.rows), self.rows)
        part = self.buffer.at[block, pl.ds(0, self.slots), rows, :]
        target = self.place + (1 if direction else -1)
        return remote(
            part,
            part,
            self.send.at[direction, step, chunk],
            self.receive.at[direction, step, chunk],
            **{self.axis: target},
        )

    def sends(self, step, act):
        pl.when((self.place > 0) & (self.place + step < self.size))(
            lambda: act(0, self.place + step)
        )
        pl.when((self.place < self.size - 1) & (self.place - step >= 0))(
            lambda: act(1, self.place - step)
        )

    def start(self, chunk):
        self.sends(0, lambda direction, block: self.copy(direction, 0, chunk, block).start())

    def tick(self, step, chunk):
        def arrive(direction, block):
            self.copy(direction, step, chunk, block).wait_recv()

        pl.when(self.place + step + 1 < self.size)(lambda: arrive(0, self.place + step + 1))
        pl.when(self.place - step - 1 >= 0)(lambda: arrive(1, self.place - step - 1))

        @pl.when(step + 1 < self.size - 1)
        def _():
            self.sends(
                step + 1,
                lambda direction, block: self.copy(direction, step + 1, chunk, block).start(),
            )

    def finish(self):
        def one(index, carry):
            step, chunk = index // chunk_count, index % chunk_count
            self.sends(
                step, lambda direction, block: self.copy(direction, step, chunk, block).wait_send()
            )
            return carry

        lax.fori_loop(0, (self.size - 1) * chunk_count, one, 0)

    def block_at(self, position):
        first = self.place + 1 - 2 * (self.place // (self.size - 1))
        last = (self.size - 1) * (1 - self.place // (self.size // 2))
        third = self.size * (self.size - 1) // 2 - self.place - first - last
        return (
            jnp.where(position == 0, self.place, 0)
            + jnp.where(position == 1, first, 0)
            + jnp.where(position == 2, third, 0)
            + jnp.where(position == 3, last, 0)
        )


class Square:
    def __init__(self, axis, buffer, slots, send, receive):
        self.axis, self.buffer, self.slots = axis, buffer, slots
        self.place = lax.axis_index(axis)
        self.near = self.place + 1 - 2 * (self.place % 2)
        self.far = (self.place + 2) % 4
        self.send, self.receive = send, receive
        self.rows = buffer.shape[2] // chunk_count

    def copy(self, kind, chunk, sending):
        rows = pl.ds(pl.multiple_of(chunk * self.rows, self.rows), self.rows)
        if kind == 0:
            block, target = (self.place if sending else self.far), self.far
        elif kind == 1:
            block, target = (self.place if sending else self.near), self.near
        else:
            block, target = (self.far if sending else (self.near + 2) % 4), self.near
        part = self.buffer.at[block, pl.ds(0, self.slots), rows, :]
        return remote(
            part, part, self.send.at[kind, chunk], self.receive.at[kind, chunk], **{self.axis: target}
        )

    def start(self, chunk):
        self.copy(0, chunk, True).start()
        self.copy(1, chunk, True).start()

    def tick(self, chunk):
        self.copy(0, chunk, False).wait_recv()
        self.copy(2, chunk, True).start()

    def arrive(self, chunk):
        self.copy(1, chunk, False).wait_recv()
        self.copy(2, chunk, False).wait_recv()

    def finish(self, chunk):
        for kind in range(3):
            self.copy(kind, chunk, True).wait_send()


def each_chunk(act):
    def one(chunk, carry):
        act(chunk)
        return carry

    lax.fori_loop(0, chunk_count, one, 0)


def greet(line, square, others=()):
    barrier = pltpu.get_barrier_semaphore()

    def signal(**place):
        pl.semaphore_signal(barrier, inc=1, device_id=place, device_id_type=MESH)

    for target in (square.near, square.far):
        signal(**{square.axis: target})
    for place in others:
        signal(**place)
    before, after = line.place > 0, line.place < line.size - 1
    pl.when(before)(lambda: signal(**{line.axis: line.place - 1}))
    pl.when(after)(lambda: signal(**{line.axis: line.place + 1}))
    ends = (line.place + line.size - 1) // line.size + 1 - (line.place + 1) // line.size
    pl.semaphore_wait(barrier, 2 + len(others) + ends)


def pipeline(line, square, left, right, multiply, finish):
    def first(chunk):
        line.tick(0, chunk)
        square.tick(chunk)
        left(line.block_at(0), chunk, 1)

    each_chunk(first)
    each_chunk(square.arrive)
    line.tick(1, 0)
    right(line.block_at(0))
    multiply(True)
    line.tick(1, 1)
    left(line.block_at(1), 0, chunk_count)
    right(line.block_at(1))
    line.tick(1, 2)
    multiply(False)
    line.tick(1, 3)
    left(line.block_at(2), 0, chunk_count)
    right(line.block_at(2))
    multiply(False)
    right(line.block_at(3))

    def last(chunk):
        line.tick(line.size - 2, chunk)
        left(line.block_at(line.size - 1), chunk, 1)

        @pl.when(chunk % 2 == 1)
        def _():
            multiply(False, chunk // 2)
            finish(chunk // 2)

    each_chunk(last)
    line.finish()
    each_chunk(square.finish)


def product_kernel(
    size,
    left_hbm,
    right_hbm,
    forward_ref,
    even_ref,
    odd_ref,
    out_ref,
    left_ref,
    right_ref,
    left_digits,
    right_digits,
    totals,
    line_send,
    line_receive,
    square_send,
    square_receive,
    local_sems,
):
    slots = left_ref.shape[1]
    line = Line("col", size, left_ref, slots, line_send, line_receive)
    square = Square("row", right_ref, slots, square_send, square_receive)
    copies = (
        pltpu.make_async_copy(left_hbm, left_ref.at[line.place], local_sems.at[0]),
        pltpu.make_async_copy(right_hbm, right_ref.at[square.place], local_sems.at[1]),
    )
    for copy in copies:
        copy.start()
    greet(line, square)
    for copy in copies:
        copy.wait()
    each_chunk(lambda chunk: (line.start(chunk), square.start(chunk)))
    groups = out_ref.shape[1] // 2 // (2 * sub_rows)

    def finish(part):
        def group(index, carry):
            start = pl.multiple_of(index * 2 * sub_rows, 2 * sub_rows)
            halves = zip(
                *(
                    folded(totals, start + half * sub_rows, sub_rows)
                    for half in range(2)
                )
            )
            for parity, (table_ref, parts) in enumerate(zip((even_ref, odd_ref), halves)):
                values = as_short(jnp.concatenate(spread_dot(table_ref[...], parts), axis=1))
                for place in range(values.shape[0]):
                    out_ref[2 * place + parity, pl.ds(start, 2 * sub_rows), :] = values[place]
            return carry

        lax.fori_loop(part * groups, (part + 1) * groups, group, 0)

    pipeline(
        line,
        square,
        lambda *place: transform_left(forward_ref, left_ref, *place, left_digits),
        lambda block: transform_right(forward_ref, right_ref, block, right_digits),
        lambda *place: multiply_points(left_digits, right_digits, totals, *place),
        finish,
    )


def result_kernel(
    size,
    product_hbm,
    upper_table,
    lower_table,
    even_ref,
    odd_ref,
    out_ref,
    left_ref,
    right_ref,
    left_digits,
    right_digits,
    totals,
    line_send,
    line_receive,
    square_send,
    square_receive,
    cross_send,
    cross_receive,
    local_sems,
):
    left_slots, right_slots = left_ref.shape[1] - 1, right_ref.shape[1] - 1
    rows = left_ref.shape[2]
    line = Line("col", size, left_ref, left_slots, line_send, line_receive)
    square = Square("row", right_ref, right_slots, square_send, square_receive)
    side = lax.axis_index("pt")
    own_left = product_hbm.at[pl.ds(0, left_slots), pl.ds(0, rows), :]
    own_right = product_hbm.at[pl.ds(right_ref.shape[1], right_slots), :, :]
    copy_left = pltpu.make_async_copy(
        own_left, left_ref.at[line.place, pl.ds(0, left_slots)], local_sems.at[0]
    )
    copy_right = pltpu.make_async_copy(
        own_right, right_ref.at[square.place, pl.ds(0, right_slots)], local_sems.at[1]
    )
    pl.when(side == 0)(copy_left.start)
    pl.when(side == 1)(copy_right.start)
    for block in range(size):
        left_ref[block, left_slots] = jnp.zeros(left_ref.shape[2:], left_ref.dtype)
        right_ref[block, right_slots] = jnp.zeros(right_ref.shape[2:], right_ref.dtype)
    greet(line, square, ({"pt": 1 - side},))

    def cross_left(chunk):
        part = pl.multiple_of(chunk * line.rows, line.rows)
        return remote(
            product_hbm.at[pl.ds(0, left_slots), pl.ds(rows + part, line.rows), :],
            left_ref.at[line.place, pl.ds(0, left_slots), pl.ds(part, line.rows), :],
            cross_send.at[chunk],
            cross_receive.at[chunk],
            pt=1 - side,
        )

    def cross_right(chunk):
        part = pl.multiple_of(chunk * square.rows, square.rows)
        return remote(
            product_hbm.at[
                pl.ds(right_ref.shape[1], right_slots), pl.ds(part, square.rows), :
            ],
            right_ref.at[square.place, pl.ds(0, right_slots), pl.ds(part, square.rows), :],
            cross_send.at[chunk],
            cross_receive.at[chunk],
            pt=1 - side,
        )

    @pl.when(side == 0)
    def _():
        each_chunk(lambda chunk: cross_left(chunk).start())
        copy_left.wait()
        each_chunk(line.start)
        each_chunk(lambda chunk: (cross_right(chunk).wait_recv(), square.start(chunk)))

    @pl.when(side == 1)
    def _():
        each_chunk(lambda chunk: cross_right(chunk).start())
        copy_right.wait()
        each_chunk(square.start)
        each_chunk(lambda chunk: (cross_left(chunk).wait_recv(), line.start(chunk)))

    groups = out_ref.shape[1] // 2 // (2 * sub_rows)

    def finish(part):
        def group(index, carry):
            start = pl.multiple_of(index * 2 * sub_rows, 2 * sub_rows)
            halves = zip(
                *(
                    folded(totals, start + half * sub_rows, sub_rows)
                    for half in range(2)
                )
            )
            for parity, (table_ref, parts) in enumerate(zip((even_ref, odd_ref), halves)):
                values = as_short(jnp.concatenate(spread_dot(table_ref[...], parts), axis=1))
                for place in range(values.shape[0]):
                    out_ref[2 * place + parity, pl.ds(start, 2 * sub_rows), :] = values[place]
            return carry

        lax.fori_loop(part * groups, (part + 1) * groups, group, 0)

    pipeline(
        line,
        square,
        lambda *place: transform_left(upper_table, left_ref, *place, left_digits),
        lambda block: transform_right(lower_table, right_ref, block, right_digits),
        lambda *place: multiply_points(left_digits, right_digits, totals, *place),
        finish,
    )
    pl.when(side == 0)(lambda: each_chunk(lambda chunk: cross_left(chunk).wait_send()))
    pl.when(side == 1)(lambda: each_chunk(lambda chunk: cross_right(chunk).wait_send()))


def call(kernel, collective_id, arguments, tables, out_shape, shapes, extra=()):
    left, right, points = shapes
    size, rows, columns = left[0], left[2], left[3]
    inner, width = right[2], right[3]
    return pl.pallas_call(
        functools.partial(kernel, size),
        out_shape=jax.ShapeDtypeStruct(out_shape, jnp.int16),
        in_specs=[pl.BlockSpec(memory_space=pl.ANY)] * len(arguments)
        + [pl.BlockSpec(memory_space=pltpu.VMEM)] * len(tables),
        out_specs=pl.BlockSpec(memory_space=pltpu.VMEM),
        scratch_shapes=[
            pltpu.VMEM(left, jnp.int16),
            pltpu.VMEM(right, jnp.int16),
            pltpu.VMEM((points, rows, 2 * columns), jnp.bfloat16),
            pltpu.VMEM((points, 2 * inner, 2 * width), jnp.bfloat16),
            pltpu.VMEM((points, rows, 2 * width), jnp.float32),
            pltpu.SemaphoreType.DMA((2, size - 1, chunk_count)),
            pltpu.SemaphoreType.DMA((2, size - 1, chunk_count)),
            pltpu.SemaphoreType.DMA((3, chunk_count)),
            pltpu.SemaphoreType.DMA((3, chunk_count)),
            *extra,
            pltpu.SemaphoreType.DMA((2,)),
        ],
        compiler_params=pltpu.CompilerParams(
            collective_id=collective_id, has_side_effects=True, vmem_limit_bytes=vmem_limit
        ),
        name=kernel.__name__,
    )(*arguments, *tables)


def square_local(first_factors, second_factors):
    size = lax.axis_size("col")
    slots, rows, columns = first_factors.shape
    points = 2 * slots
    inverse_one = make_table(points, points, points, True)
    left, right = (centre(values).astype(jnp.int16) for values in (first_factors, second_factors))
    products = call(
        product_kernel,
        0,
        (left, right),
        [
            spread_table(make_table(points, points, slots, False)),
            spread_table(inverse_one[0::2, :slots]),
            spread_table(inverse_one[1::2, :slots]),
        ],
        (points, rows, columns),
        ((size, slots, rows, columns), (size, slots, rows, columns), points),
    )
    last_points = 3 * slots
    inverse_two = make_table(last_points, last_points - 3, last_points, True)
    half = last_points // 2
    own_rows = rows // lax.axis_size("pt")
    result = call(
        result_kernel,
        1,
        (products,),
        [
            spread_table(make_table(last_points, last_points, points, False)),
            spread_table(make_table(last_points, last_points, slots, False)),
            spread_table(inverse_two[0::2, :half]),
            spread_table(inverse_two[1::2, :half]),
        ],
        (last_points - 3, own_rows, columns),
        ((size, points, own_rows, columns), (size, slots, rows, columns), last_points),
        extra=(
            pltpu.SemaphoreType.DMA((chunk_count,)),
            pltpu.SemaphoreType.DMA((chunk_count,)),
        ),
    )
    result = result.astype(jnp.float32)
    return jnp.where(result < 0.0, result + 12289.0, result) / 12289.0


def solution(mesh):
    in_specs = (P("pt", "row", "col"), P("pt", "row", "col"))
    out_specs = P(None, ("row", "pt"), "col")
    squares = mesh.shape["row"] == 4 and mesh.shape["col"] == 4 and mesh.shape["pt"] == 2
    body = square_local if squares else local
    return jax.shard_map(body, mesh=mesh, in_specs=in_specs, out_specs=out_specs, check_vma=False)
```

```python
import functools

import jax
import jax.numpy as jnp
import numpy as np
from jax import lax
from jax.experimental import pallas as pl
from jax.experimental.pallas import tpu as pltpu
from jax.sharding import PartitionSpec as P

DEG = 16


modulus = 12289
digit_base = 128


def primitive_root():
    for candidate in range(2, modulus):
        if pow(candidate, 6144, modulus) != 1 and pow(candidate, 4096, modulus) != 1:
            return candidate
    return 0


def make_table(order_size, row_count, column_count, inverse):
    generator = primitive_root()
    root_value = pow(generator, (modulus - 1) // order_size, modulus)
    scaling = 1
    if inverse:
        root_value = pow(root_value, modulus - 2, modulus)
        scaling = pow(order_size, modulus - 2, modulus)
    entries = [
        [
            pow(root_value, row_index * column_index % order_size, modulus) * scaling % modulus
            for column_index in range(column_count)
        ]
        for row_index in range(row_count)
    ]
    return np.array(entries, dtype=np.int64)


def value_digits(values):
    high_digit = values // digit_base
    return (
        high_digit.astype(jnp.bfloat16),
        (values - digit_base * high_digit).astype(jnp.bfloat16),
    )


def combine(high_high, high_low, low_high, low_low):
    top_part = high_high.astype(jnp.int32) % modulus
    middle_part = (high_low.astype(jnp.int32) + low_high.astype(jnp.int32)) % modulus
    return (
        top_part * (digit_base * digit_base) % modulus
        + middle_part * digit_base
        + low_low.astype(jnp.int32)
    ) % modulus


def transform(matrix_table, coefs):
    slot_count = coefs.shape[0]
    flat_coefs = coefs.reshape(slot_count, -1)
    table_high = jnp.asarray(matrix_table // digit_base, dtype=jnp.bfloat16)
    table_low = jnp.asarray(matrix_table % digit_base, dtype=jnp.bfloat16)
    data_high, data_low = value_digits(flat_coefs)

    def product_of(left_part, right_part):
        return jnp.dot(left_part, right_part, preferred_element_type=jnp.float32)

    mixed_values = combine(
        product_of(table_high, data_high),
        product_of(table_high, data_low),
        product_of(table_low, data_high),
        product_of(table_low, data_low),
    )
    return mixed_values.reshape(matrix_table.shape[0], coefs.shape[1], coefs.shape[2])


def batched_product(left_part, right_part):
    return jnp.einsum("bik,bkj->bij", left_part, right_part, preferred_element_type=jnp.float32)


def digit_sum(totals, left_digits, right_digits):
    return (
        totals[0] + batched_product(left_digits[0], right_digits[0]),
        totals[1] + batched_product(left_digits[0], right_digits[1]),
        totals[2] + batched_product(left_digits[1], right_digits[0]),
        totals[3] + batched_product(left_digits[1], right_digits[1]),
    )


def pointwise(left_values, right_values):
    left_points, right_points = (
        lax.all_to_all(
            lax.all_to_all(
                left_values.astype(jnp.float32), "col", split_axis=0, concat_axis=2, tiled=True
            ),
            "pt",
            split_axis=0,
            concat_axis=1,
            tiled=True,
        ),
        lax.all_to_all(
            lax.all_to_all(
                right_values.astype(jnp.float32), "col", split_axis=0, concat_axis=2, tiled=True
            ),
            "pt",
            split_axis=0,
            concat_axis=1,
            tiled=True,
        ),
    )
    left_digits = value_digits(left_points.astype(jnp.int32))
    right_digits = value_digits(right_points.astype(jnp.int32))
    zeros_init = jnp.zeros(left_points.shape, jnp.float32)
    column_parts = tuple((digit_part for digit_part in left_digits))
    totals = digit_sum(
        (zeros_init, zeros_init, zeros_init, zeros_init),
        column_parts,
        (
            lax.all_gather(right_digits[0], "row", axis=1, tiled=True),
            lax.all_gather(right_digits[1], "row", axis=1, tiled=True),
        ),
    )
    product_values = combine(totals[0], totals[1], totals[2], totals[3]).astype(jnp.float32)
    arrived = lax.all_to_all(
        lax.all_to_all(product_values, "col", split_axis=2, concat_axis=0, tiled=True),
        "pt",
        split_axis=1,
        concat_axis=0,
        tiled=True,
    )
    col_count = lax.axis_size("col")
    pt_count = lax.axis_size("pt")
    local_count = arrived.shape[0] // (col_count * pt_count)
    returned = arrived.reshape(pt_count, col_count, local_count, arrived.shape[1], arrived.shape[2])
    returned = returned.transpose(1, 0, 2, 3, 4).reshape(arrived.shape)
    return returned.astype(jnp.int32)


def local(first_factors, second_factors):
    forward_one = make_table(2 * DEG, 2 * DEG, DEG, False)
    inverse_one = make_table(2 * DEG, 2 * DEG, 2 * DEG, True)
    forward_two = make_table(4 * DEG, 4 * DEG, 2 * DEG, False)
    inverse_two = make_table(4 * DEG, 3 * DEG - 3, 4 * DEG, True)
    first_entries, second_entries = (
        lax.all_to_all(
            first_factors.astype(jnp.float32), "pt", split_axis=1, concat_axis=0, tiled=True
        ),
        lax.all_to_all(
            second_factors.astype(jnp.float32), "pt", split_axis=1, concat_axis=0, tiled=True
        ),
    )
    first_entries = first_entries.astype(jnp.int32)
    second_entries = second_entries.astype(jnp.int32)
    left_values = jnp.concatenate(
        [transform(forward_one, first_entries[:DEG]), transform(forward_one, first_entries[DEG:])],
        0,
    )
    right_values = jnp.concatenate(
        [
            transform(forward_one, second_entries[:DEG]),
            transform(forward_one, second_entries[DEG:]),
        ],
        0,
    )
    products = pointwise(left_values, right_values)
    first_product = transform(inverse_one, products[: 2 * DEG])
    second_product = transform(inverse_one, products[2 * DEG :])
    upper_values = transform(forward_two, first_product)
    lower_values = transform(forward_two[:, :DEG], second_product[DEG:])
    result_coefficients = transform(inverse_two, pointwise(upper_values, lower_values))
    return result_coefficients.astype(jnp.float32) / 12289.0


def reduce_centred(values):
    return values - 12289.0 * jnp.round(values * (1.0 / 12289.0))


def table_digits(matrix_table):
    centred = np.where(matrix_table > modulus // 2, matrix_table - modulus, matrix_table)
    high_digit = np.round(centred / 128.0)
    return high_digit, centred - 128.0 * high_digit


def centre(values):
    return jnp.where(values > modulus // 2, values - modulus, values)


MESH = pl.DeviceIdType.MESH
sub_rows = 8
chunk_count = 8
vmem_limit = 67_000_000


def spread_table(matrix_table):
    shifted_table = matrix_table * 128 % modulus
    parts = [table_digits(matrix_table), table_digits(shifted_table)]
    base = np.concatenate(
        [128.0 * parts[0][0], 128.0 * parts[1][0], parts[0][1], parts[1][1]], axis=1
    )
    slots = matrix_table.shape[1]
    weights = np.concatenate([np.full(slots, 65.0), np.full(slots, 97.0)] * 2)
    if np.max(np.abs(base) @ weights) >= 2.0**24:
        raise ValueError("inexact sums")
    return jnp.asarray(np.kron(base, np.eye(sub_rows)), dtype=jnp.bfloat16)


def low_and_high(values):
    high_digit = jnp.round(values * (1.0 / 128.0))
    return values - 128.0 * high_digit, high_digit


def spread_dot(table_value, parts):
    slots, rows, columns = parts[0].shape
    sides = []
    for values in parts:
        low, high = (
            digit.reshape(slots * rows, columns).astype(jnp.bfloat16)
            for digit in low_and_high(values)
        )
        sides.append(jnp.concatenate([low, high, low, high], axis=0))
    result = jnp.dot(
        table_value, jnp.concatenate(sides, axis=1), preferred_element_type=jnp.float32
    )
    return [
        reduce_centred(
            result[:, place * columns : (place + 1) * columns].reshape(-1, rows, columns)
        )
        for place in range(len(parts))
    ]


def as_float(values):
    return values.astype(jnp.int32).astype(jnp.float32)


def as_short(values):
    return values.astype(jnp.int32).astype(jnp.int16)


def transform_group(table_ref, source_ref, block, start):
    values = as_float(source_ref[block, :, pl.ds(start, 2 * sub_rows), :])
    parts = [values[:, :sub_rows], values[:, sub_rows:]]
    return jnp.concatenate(spread_dot(table_ref[...], parts), axis=1)


def transform_left(table_ref, source_ref, block, chunk, count, digits_ref):
    columns = source_ref.shape[3]
    groups = source_ref.shape[2] // chunk_count // (2 * sub_rows)

    def group(index, carry):
        start = pl.multiple_of(index * 2 * sub_rows, 2 * sub_rows)
        low, high = low_and_high(transform_group(table_ref, source_ref, block, start))
        digits_ref[:, pl.ds(start, 2 * sub_rows), :columns] = high.astype(jnp.bfloat16)
        digits_ref[:, pl.ds(start, 2 * sub_rows), columns:] = low.astype(jnp.bfloat16)
        return carry

    lax.fori_loop(chunk * groups, (chunk + count) * groups, group, 0)


def transform_right(table_ref, source_ref, block, digits_ref):
    rows, columns = source_ref.shape[2:]

    def group(index, carry):
        start = pl.multiple_of(index * 2 * sub_rows, 2 * sub_rows)
        values = transform_group(table_ref, source_ref, block, start)
        low, high = low_and_high(values)
        shifted_low = jnp.round(values * (-1.0 / 96.0))
        shifted_high = values + 96.0 * shifted_low
        top, bottom = pl.ds(start, 2 * sub_rows), pl.ds(rows + start, 2 * sub_rows)
        digits_ref[:, top, :columns] = shifted_high.astype(jnp.bfloat16)
        digits_ref[:, top, columns:] = shifted_low.astype(jnp.bfloat16)
        digits_ref[:, bottom, :columns] = high.astype(jnp.bfloat16)
        digits_ref[:, bottom, columns:] = low.astype(jnp.bfloat16)
        return carry

    lax.fori_loop(0, rows // (2 * sub_rows), group, 0)


def multiply_points(left_ref, right_ref, totals_ref, first, part=None):
    half = left_ref.shape[1] // 2
    rows = slice(None) if part is None else pl.ds(pl.multiple_of(part * half, half), half)
    unroll = 4 if part is None else 8

    def point(index, carry):
        for place in range(unroll):
            at = index * unroll + place
            product = jnp.dot(
                left_ref[at, rows, :], right_ref[at], preferred_element_type=jnp.float32
            )
            totals_ref[at, rows, :] = product if first else totals_ref[at, rows, :] + product
        return carry

    lax.fori_loop(0, left_ref.shape[0] // unroll, point, 0)


def folded(totals_ref, start, rows):
    width = totals_ref.shape[2] // 2
    high = totals_ref[:, pl.ds(start, rows), :width]
    low = totals_ref[:, pl.ds(start, rows), width:]
    values = reduce_centred(reduce_centred(high) * 128.0 + low)
    half = values.shape[0] // 2
    return values[:half] + values[half:], values[:half] - values[half:]


def remote(source, target, send, receive, **place):
    return pltpu.make_async_remote_copy(
        src_ref=source,
        dst_ref=target,
        send_sem=send,
        recv_sem=receive,
        device_id=place,
        device_id_type=MESH,
    )


class Line:
    def __init__(self, axis, size, buffer, slots, send, receive):
        self.axis, self.size, self.buffer = axis, size, buffer
        self.place = lax.axis_index(axis)
        self.slots = slots
        self.send, self.receive = send, receive
        self.rows = buffer.shape[2] // chunk_count

    def copy(self, direction, step, chunk, block):
        rows = pl.ds(pl.multiple_of(chunk * self.rows, self.rows), self.rows)
        part = self.buffer.at[block, pl.ds(0, self.slots), rows, :]
        target = self.place + (1 if direction else -1)
        return remote(
            part,
            part,
            self.send.at[direction, step, chunk],
            self.receive.at[direction, step, chunk],
            **{self.axis: target},
        )

    def sends(self, step, act):
        pl.when((self.place > 0) & (self.place + step < self.size))(
            lambda: act(0, self.place + step)
        )
        pl.when((self.place < self.size - 1) & (self.place - step >= 0))(
            lambda: act(1, self.place - step)
        )

    def start(self, chunk):
        self.sends(0, lambda direction, block: self.copy(direction, 0, chunk, block).start())

    def tick(self, step, chunk):
        def arrive(direction, block):
            self.copy(direction, step, chunk, block).wait_recv()

        pl.when(self.place + step + 1 < self.size)(lambda: arrive(0, self.place + step + 1))
        pl.when(self.place - step - 1 >= 0)(lambda: arrive(1, self.place - step - 1))

        @pl.when(step + 1 < self.size - 1)
        def _():
            self.sends(
                step + 1,
                lambda direction, block: self.copy(direction, step + 1, chunk, block).start(),
            )

    def finish(self):
        def one(index, carry):
            step, chunk = index // chunk_count, index % chunk_count
            self.sends(
                step, lambda direction, block: self.copy(direction, step, chunk, block).wait_send()
            )
            return carry

        lax.fori_loop(0, (self.size - 1) * chunk_count, one, 0)

    def block_at(self, position):
        first = self.place + 1 - 2 * (self.place // (self.size - 1))
        last = (self.size - 1) * (1 - self.place // (self.size // 2))
        third = self.size * (self.size - 1) // 2 - self.place - first - last
        return (
            jnp.where(position == 0, self.place, 0)
            + jnp.where(position == 1, first, 0)
            + jnp.where(position == 2, third, 0)
            + jnp.where(position == 3, last, 0)
        )


class Square:
    def __init__(self, axis, buffer, slots, send, receive):
        self.axis, self.buffer, self.slots = axis, buffer, slots
        self.place = lax.axis_index(axis)
        self.near = self.place + 1 - 2 * (self.place % 2)
        self.far = (self.place + 2) % 4
        self.send, self.receive = send, receive
        self.rows = buffer.shape[2] // chunk_count

    def copy(self, kind, chunk, sending):
        rows = pl.ds(pl.multiple_of(chunk * self.rows, self.rows), self.rows)
        if kind == 0:
            block, target = (self.place if sending else self.far), self.far
        elif kind == 1:
            block, target = (self.place if sending else self.near), self.near
        else:
            block, target = (self.far if sending else (self.near + 2) % 4), self.near
        part = self.buffer.at[block, pl.ds(0, self.slots), rows, :]
        return remote(
            part, part, self.send.at[kind, chunk], self.receive.at[kind, chunk], **{self.axis: target}
        )

    def start(self, chunk):
        self.copy(0, chunk, True).start()
        self.copy(1, chunk, True).start()

    def tick(self, chunk):
        self.copy(0, chunk, False).wait_recv()
        self.copy(2, chunk, True).start()

    def arrive(self, chunk):
        self.copy(1, chunk, False).wait_recv()
        self.copy(2, chunk, False).wait_recv()

    def finish(self, chunk):
        for kind in range(3):
            self.copy(kind, chunk, True).wait_send()


def each_chunk(act):
    def one(chunk, carry):
        act(chunk)
        return carry

    lax.fori_loop(0, chunk_count, one, 0)


def greet(line, square, others=()):
    barrier = pltpu.get_barrier_semaphore()

    def signal(**place):
        pl.semaphore_signal(barrier, inc=1, device_id=place, device_id_type=MESH)

    for target in (square.near, square.far):
        signal(**{square.axis: target})
    for place in others:
        signal(**place)
    before, after = line.place > 0, line.place < line.size - 1
    pl.when(before)(lambda: signal(**{line.axis: line.place - 1}))
    pl.when(after)(lambda: signal(**{line.axis: line.place + 1}))
    ends = (line.place + line.size - 1) // line.size + 1 - (line.place + 1) // line.size
    pl.semaphore_wait(barrier, 2 + len(others) + ends)


def pipeline(line, square, left, right, multiply, finish):
    def first(chunk):
        line.tick(0, chunk)
        square.tick(chunk)
        left(line.block_at(0), chunk, 1)

    each_chunk(first)
    each_chunk(square.arrive)
    quarter = chunk_count // 4

    def pass_on(index):
        def one(chunk, carry):
            line.tick(1, chunk)
            return carry

        lax.fori_loop(index * quarter, (index + 1) * quarter, one, 0)

    pass_on(0)
    right(line.block_at(0))
    multiply(True)
    pass_on(1)
    left(line.block_at(1), 0, chunk_count)
    right(line.block_at(1))
    pass_on(2)
    multiply(False)
    pass_on(3)
    left(line.block_at(2), 0, chunk_count)
    right(line.block_at(2))
    multiply(False)
    right(line.block_at(3))

    def last(chunk):
        line.tick(line.size - 2, chunk)
        left(line.block_at(line.size - 1), chunk, 1)

        half = chunk_count // 2

        @pl.when(chunk % half == half - 1)
        def _():
            multiply(False, chunk // half)
            finish(chunk // half)

    each_chunk(last)
    line.finish()
    each_chunk(square.finish)


def product_kernel(
    size,
    left_hbm,
    right_hbm,
    forward_ref,
    even_ref,
    odd_ref,
    out_ref,
    left_ref,
    right_ref,
    left_digits,
    right_digits,
    totals,
    line_send,
    line_receive,
    square_send,
    square_receive,
    staged,
    local_sems,
):
    slots = left_ref.shape[1]
    line = Line("col", size, left_ref, slots, line_send, line_receive)
    square = Square("row", right_ref, slots, square_send, square_receive)
    inputs = ((left_hbm, left_ref, line), (right_hbm, right_ref, square))

    def load(side, chunk):
        source, _, ring = inputs[side]
        rows = pl.ds(pl.multiple_of(chunk * ring.rows, ring.rows), ring.rows)
        return pltpu.make_async_copy(source.at[:, rows, :], staged.at[side], local_sems.at[side])

    load(0, 0).start()
    load(1, 0).start()
    greet(line, square)

    def own(chunk):
        for side, (_, target, ring) in enumerate(inputs):
            load(side, chunk).wait()
            rows = pl.ds(pl.multiple_of(chunk * ring.rows, ring.rows), ring.rows)
            target[ring.place, :, rows, :] = centre(staged[side]).astype(jnp.int16)
            pl.when(chunk + 1 < chunk_count)(lambda side=side: load(side, chunk + 1).start())

        @pl.when(chunk > 0)
        def _():
            line.start(chunk - 1)
            square.start(chunk - 1)

    each_chunk(own)
    line.start(chunk_count - 1)
    square.start(chunk_count - 1)
    groups = out_ref.shape[1] // 2 // (2 * sub_rows)

    def finish(part):
        def group(index, carry):
            start = pl.multiple_of(index * 2 * sub_rows, 2 * sub_rows)
            halves = zip(
                *(
                    folded(totals, start + half * sub_rows, sub_rows)
                    for half in range(2)
                )
            )
            for parity, (table_ref, parts) in enumerate(zip((even_ref, odd_ref), halves)):
                values = as_short(jnp.concatenate(spread_dot(table_ref[...], parts), axis=1))
                for place in range(values.shape[0]):
                    out_ref[2 * place + parity, pl.ds(start, 2 * sub_rows), :] = values[place]
            return carry

        lax.fori_loop(part * groups, (part + 1) * groups, group, 0)

    pipeline(
        line,
        square,
        lambda *place: transform_left(forward_ref, left_ref, *place, left_digits),
        lambda block: transform_right(forward_ref, right_ref, block, right_digits),
        lambda *place: multiply_points(left_digits, right_digits, totals, *place),
        finish,
    )


def result_kernel(
    size,
    product_hbm,
    upper_table,
    lower_table,
    even_ref,
    odd_ref,
    out_ref,
    left_ref,
    right_ref,
    left_digits,
    right_digits,
    totals,
    line_send,
    line_receive,
    square_send,
    square_receive,
    cross_send,
    cross_receive,
    local_sems,
):
    left_slots, right_slots = left_ref.shape[1] - 1, right_ref.shape[1] - 1
    rows = left_ref.shape[2]
    line = Line("col", size, left_ref, left_slots, line_send, line_receive)
    square = Square("row", right_ref, right_slots, square_send, square_receive)
    side = lax.axis_index("pt")
    own_left = product_hbm.at[pl.ds(0, left_slots), pl.ds(0, rows), :]
    own_right = product_hbm.at[pl.ds(right_ref.shape[1], right_slots), :, :]
    copy_left = pltpu.make_async_copy(
        own_left, left_ref.at[line.place, pl.ds(0, left_slots)], local_sems.at[0]
    )
    copy_right = pltpu.make_async_copy(
        own_right, right_ref.at[square.place, pl.ds(0, right_slots)], local_sems.at[1]
    )
    pl.when(side == 0)(copy_left.start)
    pl.when(side == 1)(copy_right.start)
    for block in range(size):
        left_ref[block, left_slots] = jnp.zeros(left_ref.shape[2:], left_ref.dtype)
        right_ref[block, right_slots] = jnp.zeros(right_ref.shape[2:], right_ref.dtype)
    greet(line, square, ({"pt": 1 - side},))

    def cross_left(chunk):
        part = pl.multiple_of(chunk * line.rows, line.rows)
        return remote(
            product_hbm.at[pl.ds(0, left_slots), pl.ds(rows + part, line.rows), :],
            left_ref.at[line.place, pl.ds(0, left_slots), pl.ds(part, line.rows), :],
            cross_send.at[chunk],
            cross_receive.at[chunk],
            pt=1 - side,
        )

    def cross_right(chunk):
        part = pl.multiple_of(chunk * square.rows, square.rows)
        return remote(
            product_hbm.at[
                pl.ds(right_ref.shape[1], right_slots), pl.ds(part, square.rows), :
            ],
            right_ref.at[square.place, pl.ds(0, right_slots), pl.ds(part, square.rows), :],
            cross_send.at[chunk],
            cross_receive.at[chunk],
            pt=1 - side,
        )

    @pl.when(side == 0)
    def _():
        each_chunk(lambda chunk: cross_left(chunk).start())
        copy_left.wait()
        each_chunk(line.start)
        each_chunk(lambda chunk: (cross_right(chunk).wait_recv(), square.start(chunk)))

    @pl.when(side == 1)
    def _():
        each_chunk(lambda chunk: cross_right(chunk).start())
        copy_right.wait()
        each_chunk(square.start)
        each_chunk(lambda chunk: (cross_left(chunk).wait_recv(), line.start(chunk)))

    groups = out_ref.shape[1] // 2 // (2 * sub_rows)

    def finish(part):
        def group(index, carry):
            start = pl.multiple_of(index * 2 * sub_rows, 2 * sub_rows)
            halves = zip(
                *(
                    folded(totals, start + half * sub_rows, sub_rows)
                    for half in range(2)
                )
            )
            for parity, (table_ref, parts) in enumerate(zip((even_ref, odd_ref), halves)):
                values = as_short(jnp.concatenate(spread_dot(table_ref[...], parts), axis=1))
                for place in range(values.shape[0]):
                    out_ref[2 * place + parity, pl.ds(start, 2 * sub_rows), :] = values[place]
            return carry

        lax.fori_loop(part * groups, (part + 1) * groups, group, 0)

    pipeline(
        line,
        square,
        lambda *place: transform_left(upper_table, left_ref, *place, left_digits),
        lambda block: transform_right(lower_table, right_ref, block, right_digits),
        lambda *place: multiply_points(left_digits, right_digits, totals, *place),
        finish,
    )
    pl.when(side == 0)(lambda: each_chunk(lambda chunk: cross_left(chunk).wait_send()))
    pl.when(side == 1)(lambda: each_chunk(lambda chunk: cross_right(chunk).wait_send()))


def call(kernel, collective_id, arguments, tables, out_shape, shapes, extra=()):
    left, right, points = shapes
    size, rows, columns = left[0], left[2], left[3]
    inner, width = right[2], right[3]
    return pl.pallas_call(
        functools.partial(kernel, size),
        out_shape=jax.ShapeDtypeStruct(out_shape, jnp.int16),
        in_specs=[pl.BlockSpec(memory_space=pl.ANY)] * len(arguments)
        + [pl.BlockSpec(memory_space=pltpu.VMEM)] * len(tables),
        out_specs=pl.BlockSpec(memory_space=pltpu.VMEM),
        scratch_shapes=[
            pltpu.VMEM(left, jnp.int16),
            pltpu.VMEM(right, jnp.int16),
            pltpu.VMEM((points, rows, 2 * columns), jnp.bfloat16),
            pltpu.VMEM((points, 2 * inner, 2 * width), jnp.bfloat16),
            pltpu.VMEM((points, rows, 2 * width), jnp.float32),
            pltpu.SemaphoreType.DMA((2, size - 1, chunk_count)),
            pltpu.SemaphoreType.DMA((2, size - 1, chunk_count)),
            pltpu.SemaphoreType.DMA((3, chunk_count)),
            pltpu.SemaphoreType.DMA((3, chunk_count)),
            *extra,
            pltpu.SemaphoreType.DMA((2,)),
        ],
        compiler_params=pltpu.CompilerParams(
            collective_id=collective_id, has_side_effects=True, vmem_limit_bytes=vmem_limit
        ),
        name=kernel.__name__,
    )(*arguments, *tables)


def square_local(first_factors, second_factors):
    size = lax.axis_size("col")
    slots, rows, columns = first_factors.shape
    points = 2 * slots
    inverse_one = make_table(points, points, points, True)
    products = call(
        product_kernel,
        0,
        (first_factors, second_factors),
        [
            spread_table(make_table(points, points, slots, False)),
            spread_table(inverse_one[0::2, :slots]),
            spread_table(inverse_one[1::2, :slots]),
        ],
        (points, rows, columns),
        ((size, slots, rows, columns), (size, slots, rows, columns), points),
        extra=(pltpu.VMEM((2, slots, rows // chunk_count, columns), jnp.int32),),
    )
    last_points = 3 * slots
    inverse_two = make_table(last_points, last_points - 3, last_points, True)
    half = last_points // 2
    own_rows = rows // lax.axis_size("pt")
    result = call(
        result_kernel,
        1,
        (products,),
        [
            spread_table(make_table(last_points, last_points, points, False)),
            spread_table(make_table(last_points, last_points, slots, False)),
            spread_table(inverse_two[0::2, :half]),
            spread_table(inverse_two[1::2, :half]),
        ],
        (last_points - 3, own_rows, columns),
        ((size, points, own_rows, columns), (size, slots, rows, columns), last_points),
        extra=(
            pltpu.SemaphoreType.DMA((chunk_count,)),
            pltpu.SemaphoreType.DMA((chunk_count,)),
        ),
    )
    result = result.astype(jnp.float32)
    return jnp.where(result < 0.0, result + 12289.0, result) / 12289.0


def solution(mesh):
    in_specs = (P("pt", "row", "col"), P("pt", "row", "col"))
    out_specs = P(None, ("row", "pt"), "col")
    squares = mesh.shape["row"] == 4 and mesh.shape["col"] == 4 and mesh.shape["pt"] == 2
    body = square_local if squares else local
    return jax.shard_map(body, mesh=mesh, in_specs=in_specs, out_specs=out_specs, check_vma=False)
```
